32 devices in a mesh: shard: 16 (over z, y, x), mp: 2 (over core).
Axes of the slice: x: 2, y: 2, z: 4, core: 2. Of those that a mesh axis runs over, the one named last changes fastest.
Arguments:
- item_rows: float32 [4096, 256], P('shard', 'mp'), may hold values from -6 to 6
- first_moment: float32 [4096, 256], P('shard', 'mp'), may hold values from -2 to 2
- second_moment: float32 [4096, 256], P('shard', 'mp'), may hold values from 0.01 to 4
- item_cot: bfloat16 [4096, 256], P('shard', 'mp'), may hold values from -6 to 6
- tile_bits: int32 [256, 8, 128], P('shard'), may hold values from 0 to 65535, as said below
- tile_item: int32 [256], P('shard'), may hold values from 0 to 1
- tile_dest: int32 [256], P('shard'), may hold values from 0 to 15
- basket_gain: float32 [256], replicated, may hold values from 0.1 to 1.9
- item_gain: float32 [256], replicated, may hold values from 0.1 to 1.9
- gate_basket: bfloat16 [256, 2048], P(None, 'mp'), may hold values from -0.375 to 0.375
- up_basket: bfloat16 [256, 2048], P(None, 'mp'), may hold values from -0.375 to 0.375
- down_basket: bfloat16 [2048, 256], P('mp'), may hold values from -0.125 to 0.125
- gate_item: bfloat16 [256, 2048], P(None, 'mp'), may hold values from -0.375 to 0.375
- up_item: bfloat16 [256, 2048], P(None, 'mp'), may hold values from -0.375 to 0.375
- down_item: bfloat16 [2048, 256], P('mp'), may hold values from -0.125 to 0.125
Outputs:
- new_rows: float32 [4096, 256], P('shard', 'mp')
- new_first: float32 [4096, 256], P('shard', 'mp')
- new_second: float32 [4096, 256], P('shard', 'mp')
The draws below stay inside these ranges and needn't reach their ends.
Inputs may be any that keep to these rules, and one draw needn't show every extreme that they name: `tile_bits`: each word holds 16 independent incidence bits in its low bits.
All inputs are finite; a program needn't handle non-finite values.
Results may differ from the reference program's by a relative error of at most 0.007.
Values may be sent and summed in bfloat16 or wider, within the bound.
No kernel may reach another device: no remote copies, remote signals or barrier semaphores. Data moves between devices by JAX's collectives and lax.ppermute only.
A program may use at most 128 MiB of HBM per device.

```python
import math
import jax
import jax.numpy as jnp
import numpy as np
from jax import lax

D = 256
FF = 2048
BLOCK = 128
ITEM_BLOCKS = 2
TILE_DEV = 16
WORDS = 8
TILES = 256
BASKET_BLOCKS = 16
ITEMS = 4096
N_SHARD = 16


def draw_tile_bits(key, part):
    return jax.random.randint(key, (TILES, WORDS, BLOCK), 0, 65536, dtype=jnp.int32)


def touch_ends(values, rng, least, largest):
    dims = values.shape
    spot = [jax.random.randint(jax.random.fold_in(rng, axis), (), 0, dims[axis]) for axis in range(len(dims))]
    values = values.at[tuple(spot)].set(least)
    longest = dims.index(max(dims))
    spot[longest] = (spot[longest] + 1) % dims[longest]
    return values.at[tuple(spot)].set(largest)


def steps_of(own_key, shape, shards, least, high):
    def one(position, parts):
        steps = jax.random.uniform(jax.random.fold_in(jax.random.fold_in(own_key, 6), position), (parts,), jnp.float32, least / len(shards), high / len(shards))
        return jnp.repeat(jnp.exp(steps), shape[position] // parts).reshape((-1,) + (1,) * (len(shape) - position - 1))

    level = one(*shards[0])
    for cut in shards[1:]:
        level = level * one(*cut)
    return level


def rank_table(amount, skew):
    portions = [(1 << 20) // math.isqrt(standing ** skew) + 1 for standing in range(1, amount + 1)]
    scale = 1 + sum(portions) // (1 << 30)
    return np.cumsum(np.array([max(1, weight // scale) for weight in portions]))


def ranked_ids(key, dims, count, skew):
    grid = rank_table(count, skew)
    pick = jax.random.randint(jax.random.fold_in(key, 1), dims, 0, int(grid[count - 1]))
    rank = jnp.searchsorted(jnp.asarray(grid, jnp.int32), pick, side="right")
    return jax.random.permutation(jax.random.fold_in(key, 2), count)[rank].astype(jnp.int32)


def gaussian(own_key, extent, deviation, reach, pieces=(), kind=jnp.bfloat16):
    values = jax.random.normal(own_key, extent, jnp.float32) * deviation
    if len(pieces) > 0:
        values = steps_of(own_key, extent, pieces, -0.22, 0.18) * values
    return jnp.clip(values, min=-reach, max=reach).astype(kind)


def setup_inputs(seed: int = 0) -> dict:
    splits = jax.random.split(jax.random.key(seed), 16)
    item_rows = gaussian(splits[0], (ITEMS, D), 1.0, 6.0, ((0, 16), (1, 2)), jnp.float32)
    first_moment = gaussian(splits[1], (ITEMS, D), 0.3, 2.0, ((0, 16), (1, 2)), jnp.float32)
    second_moment = jnp.clip(jnp.exp(math.log(4.0) - 5.9914646 * jax.random.uniform(splits[2], (ITEMS, D), jnp.float32) ** steps_of(splits[2], (ITEMS, D), ((0, 16), (1, 2)), -0.2, 0.2)), 0.01, 4.0)
    item_cot = gaussian(splits[3], (ITEMS, D), 1.0, 6.0, ((0, 16), (1, 2)))
    tile_bits = draw_tile_bits(jax.random.fold_in(splits[15], 71), 0)
    tile_item = touch_ends(ranked_ids(splits[5], (TILES,), ITEM_BLOCKS, 2), jax.random.fold_in(splits[5], 3), 0, ITEM_BLOCKS - 1).astype(jnp.int32)
    tile_dest = touch_ends(ranked_ids(splits[6], (TILES,), BASKET_BLOCKS, 2), jax.random.fold_in(splits[6], 3), 0, BASKET_BLOCKS - 1).astype(jnp.int32)
    basket_gain = jnp.clip(1.0 + 0.18 * jax.random.normal(splits[7], (D,), jnp.float32), 0.1, 1.9)
    item_gain = jnp.clip(1.0 + 0.18 * jax.random.normal(splits[8], (D,), jnp.float32), 0.1, 1.9)
    gate_basket = gaussian(splits[9], (D, FF), D ** -0.5, 0.375, ((1, 2),))
    up_basket = gaussian(splits[10], (D, FF), D ** -0.5, 0.375, ((1, 2),))
    down_basket = gaussian(splits[11], (FF, D), FF ** -0.5, 0.125, ((0, 2),))
    gate_item = gaussian(splits[12], (D, FF), D ** -0.5, 0.375, ((1, 2),))
    up_item = gaussian(splits[13], (D, FF), D ** -0.5, 0.375, ((1, 2),))
    down_item = gaussian(splits[14], (FF, D), FF ** -0.5, 0.125, ((0, 2),))
    return {"item_rows": item_rows, "first_moment": first_moment, "second_moment": second_moment, "item_cot": item_cot, "tile_bits": tile_bits, "tile_item": tile_item, "tile_dest": tile_dest, "basket_gain": basket_gain, "item_gain": item_gain, "gate_basket": gate_basket, "up_basket": up_basket, "down_basket": down_basket, "gate_item": gate_item, "up_item": up_item, "down_item": down_item}


NORM_EPSILON = 1e-05
LEARNING_RATE = 0.01
BETA_FIRST = 0.9
BETA_SECOND = 0.99
ADAM_EPSILON = 1e-08

def unpack_tiles(packed):
    shifts = jnp.arange(16, dtype=jnp.int32)
    bit_values = jnp.right_shift(packed[:, :, None, :], shifts[None, None, :, None]) & 1
    return bit_values.reshape(packed.shape[0], packed.shape[1] * 16, packed.shape[2]).astype(jnp.bfloat16)

def silu_parts(gate_values):
    sigmoid = jax.nn.sigmoid(gate_values)
    return (gate_values * sigmoid, sigmoid * (1.0 + gate_values * (1.0 - sigmoid)))

def rms_scale(values):
    return lax.rsqrt(lax.optimization_barrier(jnp.mean(values * values, axis=-1, keepdims=True)) + NORM_EPSILON)

def reference(item_rows, first_moment, second_moment, item_cot, tile_bits, tile_item, tile_dest, basket_gain, item_gain, gate_basket, up_basket, down_basket, gate_item, up_item, down_item):
    packed_all = tile_bits.reshape(N_SHARD, TILE_DEV, BLOCK // 16, BLOCK)
    item_index = tile_item.reshape(N_SHARD, TILE_DEV).astype(jnp.int32)
    dest_index = tile_dest.reshape(N_SHARD, TILE_DEV).astype(jnp.int32)

    def owner_sum(source):

        def add_device(total, inputs):
            packed_dev, item_dev, dest_dev, source_dev = inputs
            masks = unpack_tiles(packed_dev).astype(jnp.float32)
            picked = jnp.take(source_dev, item_dev, axis=0).astype(jnp.float32)
            partial_sums = jnp.einsum('tib,tif->tbf', masks, picked)
            return (total + jax.ops.segment_sum(partial_sums, dest_dev, num_segments=N_SHARD), None)
        start_total = jnp.zeros((N_SHARD, BLOCK, D), jnp.float32)
        total, unused = lax.scan(add_device, start_total, (packed_all, item_index, dest_index, source))
        return total.reshape(N_SHARD * BLOCK, D)

    def owner_spread(blocks):
        blocks = blocks.reshape(N_SHARD, BLOCK, D)

        def one_device(inputs):
            packed_dev, item_dev, dest_dev = inputs
            masks = unpack_tiles(packed_dev).astype(jnp.float32)
            selected = jnp.take(blocks, dest_dev, axis=0).astype(jnp.float32)
            contrib = jnp.einsum('tib,tbf->tif', masks, selected)
            return jax.ops.segment_sum(contrib, item_dev, num_segments=ITEM_BLOCKS)
        spread = lax.map(one_device, (packed_all, item_index, dest_index))
        return spread.reshape(N_SHARD * ITEM_BLOCKS * BLOCK, D)
    rows_bf = item_rows.astype(jnp.bfloat16).reshape(N_SHARD, ITEM_BLOCKS, BLOCK, D)
    basket_sum = owner_sum(rows_bf)
    scale_basket = rms_scale(basket_sum)
    normed = basket_sum * scale_basket * basket_gain
    normed_bf = normed.astype(jnp.bfloat16)
    gate_pre = jnp.dot(normed_bf, gate_basket, preferred_element_type=jnp.float32)
    up_pre = jnp.dot(normed_bf, up_basket, preferred_element_type=jnp.float32)
    silu_value, silu_slope = silu_parts(gate_pre)
    hidden = (silu_value * up_pre).astype(jnp.bfloat16)
    basket_out = (normed + jnp.dot(hidden, down_basket, preferred_element_type=jnp.float32)).astype(jnp.bfloat16)
    message = owner_spread(basket_out)

    def item_backward(inputs):
        message_dev, cot_dev = inputs
        scale_item = rms_scale(message_dev)
        query = (message_dev * scale_item * item_gain).astype(jnp.bfloat16)
        gate_item_pre = jnp.dot(query, gate_item, preferred_element_type=jnp.float32)
        up_item_pre = jnp.dot(query, up_item, preferred_element_type=jnp.float32)
        item_value, item_slope = silu_parts(gate_item_pre)
        grad_hidden = jnp.dot(cot_dev, down_item.T, preferred_element_type=jnp.float32)
        grad_up = (grad_hidden * item_value).astype(jnp.bfloat16)
        grad_gate = (grad_hidden * up_item_pre * item_slope).astype(jnp.bfloat16)
        grad_query = jnp.dot(grad_gate, gate_item.T, preferred_element_type=jnp.float32) + jnp.dot(grad_up, up_item.T, preferred_element_type=jnp.float32)
        inner = lax.optimization_barrier(jnp.sum(item_gain * grad_query * message_dev, axis=1, keepdims=True))
        cubed = scale_item * scale_item * scale_item
        grad_message = scale_item * item_gain * grad_query - message_dev * cubed * inner / D
        return grad_message.astype(jnp.bfloat16)
    grad_message = lax.map(item_backward, (message.reshape(N_SHARD, ITEM_BLOCKS * BLOCK, D), item_cot.reshape(N_SHARD, ITEM_BLOCKS * BLOCK, D)))
    grad_out = owner_sum(grad_message.reshape(N_SHARD, ITEM_BLOCKS, BLOCK, D))
    grad_out_bf = grad_out.astype(jnp.bfloat16)
    grad_basket_hidden = jnp.dot(grad_out_bf, down_basket.T, preferred_element_type=jnp.float32)
    grad_basket_up = (grad_basket_hidden * silu_value).astype(jnp.bfloat16)
    grad_basket_gate = (grad_basket_hidden * up_pre * silu_slope).astype(jnp.bfloat16)
    grad_normed = grad_out + (jnp.dot(grad_basket_gate, gate_basket.T, preferred_element_type=jnp.float32) + jnp.dot(grad_basket_up, up_basket.T, preferred_element_type=jnp.float32))
    inner_basket = lax.optimization_barrier(jnp.sum(basket_gain * grad_normed * basket_sum, axis=1, keepdims=True))
    cubed_basket = scale_basket * scale_basket * scale_basket
    grad_sum = (scale_basket * basket_gain * grad_normed - basket_sum * cubed_basket * inner_basket / D).astype(jnp.bfloat16)
    back_items = owner_spread(grad_sum)
    gradient = item_cot.astype(jnp.float32) + back_items
    new_first = BETA_FIRST * first_moment + (1.0 - BETA_FIRST) * gradient
    new_second = BETA_SECOND * second_moment + (1.0 - BETA_SECOND) * gradient * gradient
    new_rows = item_rows - LEARNING_RATE * new_first / (jnp.sqrt(new_second) + ADAM_EPSILON)
    return (new_rows, new_first, new_second)
```

```python
import functools

import jax
import jax.numpy as jnp
from jax import lax
from jax.experimental import pallas as pl
from jax.experimental.pallas import tpu as pltpu
from jax.sharding import PartitionSpec as P

BLOCK = 128
GATHER = 4
CHUNK = 256

NORM_EPSILON = 1e-05
LEARNING_RATE = 0.01
BETA_FIRST = 0.9
BETA_SECOND = 0.99
ADAM_EPSILON = 1e-08


F32 = jnp.float32
BF16 = jnp.bfloat16


def sds(shape, dtype):
    return jax.ShapeDtypeStruct(shape, dtype)


def run(body, outs, smem, args, scratch=(), flops=1 << 20, name=None):
    specs = [pl.BlockSpec(memory_space=pltpu.SMEM)] * len(smem)
    specs += [pl.BlockSpec(memory_space=pltpu.VMEM)] * len(args)
    return pl.pallas_call(
        body,
        out_shape=outs,
        in_specs=specs,
        out_specs=jax.tree.map(lambda _: pl.BlockSpec(memory_space=pltpu.VMEM), outs),
        scratch_shapes=list(scratch),
        cost_estimate=pl.CostEstimate(flops=flops, bytes_accessed=1 << 20, transcendentals=0),
        name=name,
    )(*smem, *args)


def dot(a, b):
    return jnp.dot(a, b, preferred_element_type=F32)


def dot_nt(a, b):
    return lax.dot_general(a, b, (((1,), (1,)), ((), ())), preferred_element_type=F32)


def sigmoid(v):
    return 0.5 * jnp.tanh(0.5 * v) + 0.5


def pack_body(core_ref, rows_ref, words_ref, meta_ref, pack_ref, lo_ref, hi_ref, *, half):
    items = rows_ref.shape[0]
    start = pl.multiple_of(core_ref[0] * half, half)
    pack_ref[0:items, :] = rows_ref[...].astype(BF16)
    words = words_ref[...]
    lo_ref[...] = (words & 255).astype(F32).T
    hi_ref[...] = (words >> 8).astype(F32).T
    pack_ref[items : items + half, :] = lo_ref[pl.ds(start, half), :].astype(BF16)
    pack_ref[items + half : items + 2 * half, :] = hi_ref[pl.ds(start, half), :].astype(BF16)
    pack_ref[items + 2 * half :, :] = meta_ref[...]


def join_halves(core, whole_ref, own_ref_list, other_ref, rows):
    width = other_ref.shape[1]
    mine = pl.multiple_of(core * width, width)
    theirs = pl.multiple_of((1 - core) * width, width)
    for l, own in enumerate(own_ref_list):
        whole_ref[l * rows : (l + 1) * rows, pl.ds(mine, width)] = own[0:rows, :]
        whole_ref[l * rows : (l + 1) * rows, pl.ds(theirs, width)] = other_ref[
            l * rows : (l + 1) * rows, :
        ]


def sums_body(idx_ref, *refs, members, groups, half, items, tiles):
    packs = refs[:members]
    other_ref, spread_ref = refs[members : members + 2]
    mt_ref = refs[members + 2]
    out_refs = refs[members + 3 : members + 3 + groups]
    rows_ref = refs[members + 3 + groups]
    core = idx_ref[2 * members * tiles]
    mt_ref[...] = jnp.zeros_like(mt_ref)
    byte_rows = jnp.concatenate(
        [
            jnp.concatenate(
                [p[items : items + half, :], p[items + half : items + 2 * half, :]], axis=1
            )
            for p in packs
        ],
        axis=0,
    )
    shift = lax.broadcasted_iota(jnp.int32, (members * half, 2 * BLOCK), 1) % 8
    for q in range(tiles // 2):
        spread = dot(byte_rows, spread_ref[:, q * 2 * BLOCK : (q + 1) * 2 * BLOCK])
        bits = jnp.right_shift(spread.astype(jnp.int32), shift) & 1
        mask = bits.astype(F32).astype(BF16)
        for l in range(members):
            for b in range(2):
                at = 2 * (l * tiles + 2 * q + b)
                row = pl.multiple_of(idx_ref[at], half)
                lane = pl.multiple_of(idx_ref[at + 1], BLOCK)
                where = (pl.ds(row, half), pl.ds(lane, BLOCK))
                mt_ref[where] = (
                    mt_ref[where]
                    + mask[l * half : (l + 1) * half, b * BLOCK : (b + 1) * BLOCK]
                )
    join_halves(core, rows_ref, packs, other_ref, items)
    per = members * half
    for i in range(groups):
        total = dot(mt_ref[i * per : (i + 1) * per, :], rows_ref[...])
        out_refs[i][...] = total.astype(out_refs[i].dtype)


def turn_body(mt_ref, out_ref, *, items):
    for c in range(mt_ref.shape[0] // BLOCK):
        block = mt_ref[c * BLOCK : (c + 1) * BLOCK, 0:items].astype(F32)
        out_ref[:, c * BLOCK : (c + 1) * BLOCK] = block.T.astype(BF16)


def add_all(refs):
    total = refs[0][...].astype(F32)
    for r in refs[1:]:
        total = total + r[...].astype(F32)
    return total


def rms(values):
    return lax.rsqrt(jnp.mean(values * values, axis=-1, keepdims=True) + NORM_EPSILON)


def halves(own_ref, other_ref, axis):
    for ref in (own_ref, other_ref):
        for c in range(ref.shape[axis] // CHUNK):
            yield ref, c * CHUNK


def basket_body(*refs, groups):
    parts = refs[:groups]
    gain_ref, gate_a, gate_b, up_a, up_b, down_a, down_b = refs[groups : groups + 7]
    out_ref, sum_ref, value_ref, slope_ref = refs[groups + 7 :]
    total = add_all(parts)
    sum_ref[...] = total
    normed = total * rms(total) * gain_ref[...]
    normed_bf = normed.astype(BF16)
    acc = normed
    at = 0
    for gate, up, down in ((gate_a, up_a, down_a), (gate_b, up_b, down_b)):
        for c in range(0, gate.shape[1], CHUNK):
            gate_pre = dot(normed_bf, gate[:, c : c + CHUNK])
            up_pre = dot(normed_bf, up[:, c : c + CHUNK])
            sig = sigmoid(gate_pre)
            value = gate_pre * sig
            acc = acc + dot((value * up_pre).astype(BF16), down[c : c + CHUNK, :])
            value_ref[:, at : at + CHUNK] = value.astype(BF16)
            slope_ref[:, at : at + CHUNK] = (up_pre * (sig + value * (1.0 - sig))).astype(BF16)
            at += CHUNK
    out_ref[...] = acc.astype(BF16)


def message_body(core_ref, mo_ref, *refs, groups):
    parts = refs[:groups]
    mine_ref, theirs_ref, all_ref = refs[groups:]
    per = parts[0].shape[0]
    total = dot(mo_ref[:, 0:per], parts[0][...])
    for i in range(1, groups):
        total = total + dot(mo_ref[:, i * per : (i + 1) * per], parts[i][...])
    all_ref[...] = total
    rows = mine_ref.shape[0]
    core = core_ref[0]
    mine_ref[...] = all_ref[pl.ds(pl.multiple_of(core * rows, rows), rows), :]
    theirs_ref[...] = all_ref[pl.ds(pl.multiple_of((1 - core) * rows, rows), rows), :]


def item_hidden_body(core_ref, mine_ref, other_ref, down_a, down_b, out_ref, cot_ref):
    core = core_ref[0]
    width = mine_ref.shape[1]
    cot_ref[:, pl.ds(pl.multiple_of(core * width, width), width)] = mine_ref[...]
    cot_ref[:, pl.ds(pl.multiple_of((1 - core) * width, width), width)] = other_ref[...]
    cot = cot_ref[...]
    at = 0
    for down in (down_a, down_b):
        for c in range(0, down.shape[0], CHUNK):
            out_ref[:, at : at + CHUNK] = dot_nt(cot, down[c : c + CHUNK, :])
            at += CHUNK


def item_body(mine_ref, other_ref, hidden_ref, gain_ref, gate_a, gate_b, up_a, up_b, out_ref):
    message = mine_ref[...] + other_ref[...]
    scale = rms(message)
    gain = gain_ref[...]
    query = (message * scale * gain).astype(BF16)
    acc = jnp.zeros_like(message)
    at = 0
    for gate, up in ((gate_a, up_a), (gate_b, up_b)):
        for c in range(0, gate.shape[1], CHUNK):
            gate_w = gate[:, c : c + CHUNK]
            up_w = up[:, c : c + CHUNK]
            gate_pre = dot(query, gate_w)
            up_pre = dot(query, up_w)
            sig = sigmoid(gate_pre)
            value = gate_pre * sig
            hidden = hidden_ref[:, at : at + CHUNK]
            grad_up = (hidden * value).astype(BF16)
            grad_gate = (hidden * up_pre * (sig + value * (1.0 - sig))).astype(BF16)
            acc = acc + dot_nt(grad_gate, gate_w) + dot_nt(grad_up, up_w)
            at += CHUNK
    weighted = gain * acc
    inner = jnp.mean(weighted * message, axis=1, keepdims=True)
    cubed = scale * scale * scale
    out_ref[...] = (scale * weighted - message * (cubed * inner)).astype(BF16)


def grad_sums_body(core_ref, mt_ref, *refs, members, groups):
    owns = refs[:members]
    other_ref = refs[members]
    out_refs = refs[members + 1 : members + 1 + groups]
    rows_ref = refs[members + 1 + groups]
    core = core_ref[0]
    rows = owns[0].shape[0]
    for l in range(members):
        mine = pl.multiple_of((2 * l + core) * rows, rows)
        theirs = pl.multiple_of((2 * l + 1 - core) * rows, rows)
        rows_ref[pl.ds(mine, rows), :] = owns[l][...]
        rows_ref[pl.ds(theirs, rows), :] = other_ref[l * rows : (l + 1) * rows, :]
    per = out_refs[0].shape[0]
    for i in range(groups):
        total = dot(mt_ref[i * per : (i + 1) * per, :], rows_ref[...])
        out_refs[i][...] = total.astype(out_refs[i].dtype)


def basket_back_body(*refs, groups):
    parts = refs[:groups]
    sum_ref, value_ref, slope_ref, gain_ref = refs[groups : groups + 4]
    gate_a, gate_b, up_a, up_b, down_a, down_b, out_ref = refs[groups + 4 :]
    grad_out = add_all(parts)
    grad_bf = grad_out.astype(BF16)
    acc = grad_out
    at = 0
    for gate, up, down in ((gate_a, up_a, down_a), (gate_b, up_b, down_b)):
        for c in range(0, gate.shape[1], CHUNK):
            hidden = dot_nt(grad_bf, down[c : c + CHUNK, :])
            grad_up = (hidden * value_ref[:, at : at + CHUNK].astype(F32)).astype(BF16)
            grad_gate = (hidden * slope_ref[:, at : at + CHUNK].astype(F32)).astype(BF16)
            acc = acc + dot_nt(grad_gate, gate[:, c : c + CHUNK])
            acc = acc + dot_nt(grad_up, up[:, c : c + CHUNK])
            at += CHUNK
    total = sum_ref[...]
    scale = rms(total)
    weighted = gain_ref[...] * acc
    inner = jnp.mean(weighted * total, axis=1, keepdims=True)
    cubed = scale * scale * scale
    out_ref[...] = (scale * weighted - total * (cubed * inner)).astype(BF16)


def back_body(core_ref, mo_ref, *refs, groups):
    parts = refs[:groups]
    mine_ref, theirs_ref, all_ref = refs[groups:]
    per = parts[0].shape[0]
    total = dot(mo_ref[:, 0:per], parts[0][...])
    for i in range(1, groups):
        total = total + dot(mo_ref[:, i * per : (i + 1) * per], parts[i][...])
    all_ref[...] = total
    width = mine_ref.shape[1]
    core = core_ref[0]
    mine_ref[...] = all_ref[:, pl.ds(pl.multiple_of(core * width, width), width)]
    theirs_ref[...] = all_ref[:, pl.ds(pl.multiple_of((1 - core) * width, width), width)]


def adam_body(back_ref, other_ref, cot_ref, rows_ref, first_ref, second_ref, r_ref, f_ref, s_ref):
    gradient = cot_ref[...].astype(F32) + (back_ref[...] + other_ref[...])
    first = BETA_FIRST * first_ref[...] + (1.0 - BETA_FIRST) * gradient
    second = BETA_SECOND * second_ref[...] + (1.0 - BETA_SECOND) * gradient * gradient
    f_ref[...] = first
    s_ref[...] = second
    r_ref[...] = rows_ref[...] - LEARNING_RATE * first / (jnp.sqrt(second) + ADAM_EPSILON)


def local(
    item_rows,
    first_moment,
    second_moment,
    item_cot,
    tile_bits,
    tile_item,
    tile_dest,
    basket_gain,
    item_gain,
    gate_basket,
    up_basket,
    down_basket,
    gate_item,
    up_item,
    down_item,
):
    shards = lax.axis_size("shard")
    members = GATHER if shards % GATHER == 0 else 1
    groups = shards // members
    items, width = item_rows.shape
    features = basket_gain.shape[0]
    tiles, words, _ = tile_bits.shape
    half = BLOCK // 2
    item_half = items // 2
    hidden = 2 * gate_basket.shape[1]
    per = members * half
    core = lax.axis_index("mp")
    place = lax.axis_index("shard") % groups
    core_arr = core.astype(jnp.int32).reshape(1)

    def swap(x):
        return lax.ppermute(x, "mp", [(0, 1), (1, 0)])

    def gather(x):
        return [
            lax.ppermute(
                x, "shard", [(s, (((s // groups) ^ k) * groups) + s % groups) for s in range(shards)]
            )
            for k in range(1, members)
        ]

    def exchange(xs):
        return [
            lax.ppermute(
                xs[k - 1],
                "shard",
                [(s, (s // groups) * groups + ((s % groups) ^ k)) for s in range(shards)],
            )
            for k in range(1, groups)
        ]

    meta = jnp.stack([tile_dest % 128, tile_dest // 128, tile_item]).astype(BF16)
    meta = jnp.pad(meta, ((0, 13), (0, width - tiles)))
    pack = run(
        functools.partial(pack_body, half=half),
        sds((items + 2 * half + 16, width), BF16),
        (core_arr,),
        (item_rows, tile_bits.reshape(tiles * words, BLOCK), meta),
        scratch=[pltpu.VMEM((BLOCK, tiles * words), F32)] * 2,
        name="pack",
    )
    packs = [pack] + gather(pack)
    rows_other = swap(jnp.concatenate([q[:items] for q in packs], axis=0))
    cot_other = swap(lax.dynamic_slice_in_dim(item_cot, (1 - core) * item_half, item_half, 0))
    cot_mine = lax.dynamic_slice_in_dim(item_cot, core * item_half, item_half, 0)
    gate_b, up_b, down_b = gate_basket, up_basket, down_basket
    gate_bo, up_bo, down_bo = swap(gate_basket), swap(up_basket), swap(down_basket)
    gate_io, up_io, down_io = swap(gate_item), swap(up_item), swap(down_item)

    metas = jnp.stack([q[items + 2 * half : items + 2 * half + 3, :tiles] for q in packs])
    metas = metas.astype(jnp.int32)
    dest = metas[:, 0] + 128 * metas[:, 1]
    row_at = (((dest % groups) ^ place) * members + dest // groups) * half
    lane_at = metas[:, 2] * BLOCK + items * jnp.arange(members, dtype=jnp.int32)[:, None]
    idx = jnp.concatenate([jnp.stack([row_at, lane_at], axis=-1).reshape(-1), core_arr])

    source = lax.broadcasted_iota(jnp.int32, (2 * tiles * words, tiles * BLOCK), 0)
    target = lax.broadcasted_iota(jnp.int32, (2 * tiles * words, tiles * BLOCK), 1)
    spread = (
        (source % (tiles * words) == target // 16) & (source // (tiles * words) == (target // 8) % 2)
    ).astype(BF16)

    part_shapes = [sds((per, features), F32)] + [sds((per, features), BF16)] * (groups - 1)
    mt, *parts = run(
        functools.partial(
            sums_body, members=members, groups=groups, half=half, items=items, tiles=tiles
        ),
        [sds((shards * half, members * items), BF16)] + part_shapes,
        (idx,),
        (*packs, rows_other, spread),
        scratch=[pltpu.VMEM((members * items, features), BF16)],
        flops=1 << 30,
        name="sums",
    )
    received = exchange(parts[1:])
    mo = run(
        functools.partial(turn_body, items=items),
        sds((items, shards * half), BF16),
        (),
        (mt,),
        flops=1 << 29,
        name="turn",
    )
    item_hidden = run(
        item_hidden_body,
        sds((item_half, hidden), F32),
        (core_arr,),
        (cot_mine, cot_other, down_item, down_io),
        scratch=[pltpu.VMEM((item_half, features), BF16)],
        flops=1 << 29,
        name="item_hidden",
    )
    basket_out, basket_sum, value, slope = run(
        functools.partial(basket_body, groups=groups),
        [
            sds((per, features), BF16),
            sds((per, features), F32),
            sds((per, hidden), BF16),
            sds((per, hidden), BF16),
        ],
        (),
        (
            parts[0],
            *received,
            basket_gain.reshape(1, features),
            gate_b,
            gate_bo,
            up_b,
            up_bo,
            down_b,
            down_bo,
        ),
        flops=1 << 30,
        name="basket",
    )
    outs = [basket_out] + exchange([basket_out] * (groups - 1))
    message_mine, message_theirs = run(
        functools.partial(message_body, groups=groups),
        [sds((item_half, features), F32)] * 2,
        (core_arr,),
        (mo, *outs),
        scratch=[pltpu.VMEM((items, features), F32)],
        flops=1 << 28,
        name="message",
    )
    message_other = swap(message_theirs)
    grad_message = run(
        item_body,
        sds((item_half, features), BF16),
        (),
        (
            message_mine,
            message_other,
            item_hidden,
            item_gain.reshape(1, features),
            gate_item,
            gate_io,
            up_item,
            up_io,
        ),
        flops=1 << 30,
        name="item",
    )
    grads = [grad_message] + gather(grad_message)
    grads_other = swap(jnp.concatenate(grads, axis=0))
    grad_parts = run(
        functools.partial(grad_sums_body, members=members, groups=groups),
        part_shapes,
        (core_arr,),
        (mt, *grads, grads_other),
        scratch=[pltpu.VMEM((members * items, features), BF16)],
        flops=1 << 29,
        name="grad_sums",
    )
    grad_received = exchange(grad_parts[1:])
    grad_sum = run(
        functools.partial(basket_back_body, groups=groups),
        sds((per, features), BF16),
        (),
        (
            grad_parts[0],
            *grad_received,
            basket_sum,
            value,
            slope,
            basket_gain.reshape(1, features),
            gate_b,
            gate_bo,
            up_b,
            up_bo,
            down_b,
            down_bo,
        ),
        flops=1 << 30,
        name="basket_back",
    )
    sums = [grad_sum] + exchange([grad_sum] * (groups - 1))
    back_mine, back_theirs = run(
        functools.partial(back_body, groups=groups),
        [sds((items, width), F32)] * 2,
        (core_arr,),
        (mo, *sums),
        scratch=[pltpu.VMEM((items, features), F32)],
        flops=1 << 28,
        name="back",
    )
    back_other = swap(back_theirs)
    new_rows, new_first, new_second = run(
        adam_body,
        [sds((items, width), F32)] * 3,
        (),
        (back_mine, back_other, item_cot, item_rows, first_moment, second_moment),
        name="adam",
    )
    return (new_rows, new_first, new_second)


def solution(mesh):
    return jax.shard_map(
        local,
        mesh=mesh,
        in_specs=(
            P("shard", "mp"),
            P("shard", "mp"),
            P("shard", "mp"),
            P("shard", "mp"),
            P("shard", None, None),
            P("shard"),
            P("shard"),
            P(),
            P(),
            P(None, "mp"),
            P(None, "mp"),
            P("mp", None),
            P(None, "mp"),
            P(None, "mp"),
            P("mp", None),
        ),
        out_specs=(P("shard", "mp"), P("shard", "mp"), P("shard", "mp")),
        check_vma=False,
    )
```

```python
import functools

import jax
import jax.numpy as jnp
import numpy as np
from jax import lax
from jax.experimental import pallas as pl
from jax.experimental.pallas import tpu as pltpu
from jax.sharding import PartitionSpec as P

BLOCK = 128
GATHER = 4
CHUNK = 256

NORM_EPSILON = 1e-05
LEARNING_RATE = 0.01
BETA_FIRST = 0.9
BETA_SECOND = 0.99
ADAM_EPSILON = 1e-08


F32 = jnp.float32
BF16 = jnp.bfloat16


def sds(shape, dtype):
    return jax.ShapeDtypeStruct(shape, dtype)


def nbytes(x):
    return int(np.prod(x.shape)) * jnp.dtype(x.dtype).itemsize


def run(body, outs, smem, args, scratch=(), flops=1 << 20, name=None):
    limit = sum(nbytes(x) for x in (*args, *jax.tree.leaves(outs), *scratch)) + (4 << 20)
    specs = [pl.BlockSpec(memory_space=pltpu.SMEM)] * len(smem)
    specs += [pl.BlockSpec(memory_space=pltpu.VMEM)] * len(args)
    return pl.pallas_call(
        body,
        out_shape=outs,
        in_specs=specs,
        out_specs=jax.tree.map(lambda _: pl.BlockSpec(memory_space=pltpu.VMEM), outs),
        scratch_shapes=list(scratch),
        cost_estimate=pl.CostEstimate(flops=flops, bytes_accessed=1 << 20, transcendentals=0),
        compiler_params=pltpu.CompilerParams(vmem_limit_bytes=min(limit, 60 * 1024 * 1024)),
        name=name,
    )(*smem, *args)


def dot(a, b):
    return jnp.dot(a, b, preferred_element_type=F32)


def dot_nt(a, b):
    return lax.dot_general(a, b, (((1,), (1,)), ((), ())), preferred_element_type=F32)


def sigmoid(v):
    return 0.5 * jnp.tanh(0.5 * v) + 0.5


def pack_body(core_ref, rows_ref, words_ref, meta_ref, pack_ref, lo_ref, hi_ref, *, half):
    items = rows_ref.shape[0]
    start = pl.multiple_of(core_ref[0] * half, half)
    pack_ref[0:items, :] = rows_ref[...].astype(BF16)
    words = words_ref[...]
    lo_ref[...] = (words & 255).astype(F32).T
    hi_ref[...] = (words >> 8).astype(F32).T
    pack_ref[items : items + half, :] = lo_ref[pl.ds(start, half), :].astype(BF16)
    pack_ref[items + half : items + 2 * half, :] = hi_ref[pl.ds(start, half), :].astype(BF16)
    pack_ref[items + 2 * half :, :] = meta_ref[...]


def join_halves(core, whole_ref, own_ref_list, other_ref, rows):
    width = other_ref.shape[1]
    mine = pl.multiple_of(core * width, width)
    theirs = pl.multiple_of((1 - core) * width, width)
    for l, own in enumerate(own_ref_list):
        whole_ref[l * rows : (l + 1) * rows, pl.ds(mine, width)] = own[0:rows, :]
        whole_ref[l * rows : (l + 1) * rows, pl.ds(theirs, width)] = other_ref[
            l * rows : (l + 1) * rows, :
        ]


def sums_body(idx_ref, *refs, members, groups, half, items, tiles):
    packs = refs[:members]
    other_ref, spread_ref = refs[members : members + 2]
    mt_ref = refs[members + 2]
    out_refs = refs[members + 3 : members + 3 + groups]
    rows_ref = refs[members + 3 + groups]
    core = idx_ref[2 * members * tiles]
    mt_ref[...] = jnp.zeros_like(mt_ref)
    byte_rows = jnp.concatenate(
        [
            jnp.concatenate(
                [p[items : items + half, :], p[items + half : items + 2 * half, :]], axis=1
            )
            for p in packs
        ],
        axis=0,
    )
    shift = lax.broadcasted_iota(jnp.int32, (members * half, 2 * BLOCK), 1) % 8
    for q in range(tiles // 2):
        spread = dot(byte_rows, spread_ref[:, q * 2 * BLOCK : (q + 1) * 2 * BLOCK])
        bits = jnp.right_shift(spread.astype(jnp.int32), shift) & 1
        mask = bits.astype(F32).astype(BF16)
        for l in range(members):
            for b in range(2):
                at = 2 * (l * tiles + 2 * q + b)
                row = pl.multiple_of(idx_ref[at], half)
                lane = pl.multiple_of(idx_ref[at + 1], BLOCK)
                where = (pl.ds(row, half), pl.ds(lane, BLOCK))
                mt_ref[where] = (
                    mt_ref[where]
                    + mask[l * half : (l + 1) * half, b * BLOCK : (b + 1) * BLOCK]
                )
    join_halves(core, rows_ref, packs, other_ref, items)
    per = members * half
    for i in range(groups):
        total = dot(mt_ref[i * per : (i + 1) * per, :], rows_ref[...])
        out_refs[i][...] = total.astype(out_refs[i].dtype)


def turn_body(mt_ref, out_ref, *, items):
    for c in range(mt_ref.shape[0] // BLOCK):
        block = mt_ref[c * BLOCK : (c + 1) * BLOCK, 0:items].astype(F32)
        out_ref[:, c * BLOCK : (c + 1) * BLOCK] = block.T.astype(BF16)


def add_all(refs):
    total = refs[0][...].astype(F32)
    for r in refs[1:]:
        total = total + r[...].astype(F32)
    return total


def rms(values):
    return lax.rsqrt(jnp.mean(values * values, axis=-1, keepdims=True) + NORM_EPSILON)


def halves(own_ref, other_ref, axis):
    for ref in (own_ref, other_ref):
        for c in range(ref.shape[axis] // CHUNK):
            yield ref, c * CHUNK


def basket_body(*refs, groups):
    parts = refs[:groups]
    gain_ref, gate_a, gate_b, up_a, up_b, down_a, down_b = refs[groups : groups + 7]
    out_ref, sum_ref, value_ref, slope_ref = refs[groups + 7 :]
    total = add_all(parts)
    sum_ref[...] = total
    normed = total * rms(total) * gain_ref[...]
    normed_bf = normed.astype(BF16)
    acc = normed
    at = 0
    for gate, up, down in ((gate_a, up_a, down_a), (gate_b, up_b, down_b)):
        for c in range(0, gate.shape[1], CHUNK):
            gate_pre = dot(normed_bf, gate[:, c : c + CHUNK])
            up_pre = dot(normed_bf, up[:, c : c + CHUNK])
            sig = sigmoid(gate_pre)
            value = gate_pre * sig
            acc = acc + dot((value * up_pre).astype(BF16), down[c : c + CHUNK, :])
            value_ref[:, at : at + CHUNK] = value.astype(BF16)
            slope_ref[:, at : at + CHUNK] = (up_pre * (sig + value * (1.0 - sig))).astype(BF16)
            at += CHUNK
    out_ref[...] = acc.astype(BF16)


def message_body(core_ref, mo_ref, *refs, groups):
    parts = refs[:groups]
    mine_ref, theirs_ref, all_ref = refs[groups:]
    per = parts[0].shape[0]
    total = dot(mo_ref[:, 0:per], parts[0][...])
    for i in range(1, groups):
        total = total + dot(mo_ref[:, i * per : (i + 1) * per], parts[i][...])
    all_ref[...] = total
    rows = mine_ref.shape[0]
    core = core_ref[0]
    mine_ref[...] = all_ref[pl.ds(pl.multiple_of(core * rows, rows), rows), :]
    theirs_ref[...] = all_ref[pl.ds(pl.multiple_of((1 - core) * rows, rows), rows), :]


def item_hidden_body(core_ref, mine_ref, other_ref, down_a, down_b, out_ref, cot_ref):
    core = core_ref[0]
    width = mine_ref.shape[1]
    cot_ref[:, pl.ds(pl.multiple_of(core * width, width), width)] = mine_ref[...]
    cot_ref[:, pl.ds(pl.multiple_of((1 - core) * width, width), width)] = other_ref[...]
    cot = cot_ref[...]
    at = 0
    for down in (down_a, down_b):
        for c in range(0, down.shape[0], CHUNK):
            out_ref[:, at : at + CHUNK] = dot_nt(cot, down[c : c + CHUNK, :])
            at += CHUNK


def item_body(mine_ref, other_ref, hidden_ref, gain_ref, gate_a, gate_b, up_a, up_b, out_ref):
    message = mine_ref[...] + other_ref[...]
    scale = rms(message)
    gain = gain_ref[...]
    query = (message * scale * gain).astype(BF16)
    acc = jnp.zeros_like(message)
    at = 0
    for gate, up in ((gate_a, up_a), (gate_b, up_b)):
        for c in range(0, gate.shape[1], CHUNK):
            gate_w = gate[:, c : c + CHUNK]
            up_w = up[:, c : c + CHUNK]
            gate_pre = dot(query, gate_w)
            up_pre = dot(query, up_w)
            sig = sigmoid(gate_pre)
            value = gate_pre * sig
            hidden = hidden_ref[:, at : at + CHUNK]
            grad_up = (hidden * value).astype(BF16)
            grad_gate = (hidden * up_pre * (sig + value * (1.0 - sig))).astype(BF16)
            acc = acc + dot_nt(grad_gate, gate_w) + dot_nt(grad_up, up_w)
            at += CHUNK
    weighted = gain * acc
    inner = jnp.mean(weighted * message, axis=1, keepdims=True)
    cubed = scale * scale * scale
    out_ref[...] = (scale * weighted - message * (cubed * inner)).astype(BF16)


def grad_sums_body(core_ref, mt_ref, *refs, members, groups):
    owns = refs[:members]
    other_ref = refs[members]
    out_refs = refs[members + 1 : members + 1 + groups]
    rows_ref = refs[members + 1 + groups]
    core = core_ref[0]
    rows = owns[0].shape[0]
    for l in range(members):
        mine = pl.multiple_of((2 * l + core) * rows, rows)
        theirs = pl.multiple_of((2 * l + 1 - core) * rows, rows)
        rows_ref[pl.ds(mine, rows), :] = owns[l][...]
        rows_ref[pl.ds(theirs, rows), :] = other_ref[l * rows : (l + 1) * rows, :]
    per = out_refs[0].shape[0]
    for i in range(groups):
        total = dot(mt_ref[i * per : (i + 1) * per, :], rows_ref[...])
        out_refs[i][...] = total.astype(out_refs[i].dtype)


def basket_back_body(*refs, groups):
    parts = refs[:groups]
    sum_ref, value_ref, slope_ref, gain_ref = refs[groups : groups + 4]
    gate_a, gate_b, up_a, up_b, down_a, down_b, out_ref = refs[groups + 4 :]
    grad_out = add_all(parts)
    grad_bf = grad_out.astype(BF16)
    acc = grad_out
    at = 0
    for gate, up, down in ((gate_a, up_a, down_a), (gate_b, up_b, down_b)):
        for c in range(0, gate.shape[1], CHUNK):
            hidden = dot_nt(grad_bf, down[c : c + CHUNK, :])
            grad_up = (hidden * value_ref[:, at : at + CHUNK].astype(F32)).astype(BF16)
            grad_gate = (hidden * slope_ref[:, at : at + CHUNK].astype(F32)).astype(BF16)
            acc = acc + dot_nt(grad_gate, gate[:, c : c + CHUNK])
            acc = acc + dot_nt(grad_up, up[:, c : c + CHUNK])
            at += CHUNK
    total = sum_ref[...]
    scale = rms(total)
    weighted = gain_ref[...] * acc
    inner = jnp.mean(weighted * total, axis=1, keepdims=True)
    cubed = scale * scale * scale
    out_ref[...] = (scale * weighted - total * (cubed * inner)).astype(BF16)


def back_body(core_ref, mo_ref, *refs, groups):
    parts = refs[:groups]
    mine_ref, theirs_ref, all_ref = refs[groups:]
    per = parts[0].shape[0]
    total = dot(mo_ref[:, 0:per], parts[0][...])
    for i in range(1, groups):
        total = total + dot(mo_ref[:, i * per : (i + 1) * per], parts[i][...])
    all_ref[...] = total
    width = mine_ref.shape[1]
    core = core_ref[0]
    mine_ref[...] = all_ref[:, pl.ds(pl.multiple_of(core * width, width), width)]
    theirs_ref[...] = all_ref[:, pl.ds(pl.multiple_of((1 - core) * width, width), width)]


def adam_body(back_ref, other_ref, cot_ref, rows_ref, first_ref, second_ref, r_ref, f_ref, s_ref):
    gradient = cot_ref[...].astype(F32) + (back_ref[...] + other_ref[...])
    first = BETA_FIRST * first_ref[...] + (1.0 - BETA_FIRST) * gradient
    second = BETA_SECOND * second_ref[...] + (1.0 - BETA_SECOND) * gradient * gradient
    f_ref[...] = first
    s_ref[...] = second
    r_ref[...] = rows_ref[...] - LEARNING_RATE * first / (jnp.sqrt(second) + ADAM_EPSILON)


def local(
    item_rows,
    first_moment,
    second_moment,
    item_cot,
    tile_bits,
    tile_item,
    tile_dest,
    basket_gain,
    item_gain,
    gate_basket,
    up_basket,
    down_basket,
    gate_item,
    up_item,
    down_item,
):
    shards = lax.axis_size("shard")
    members = GATHER if shards % GATHER == 0 else 1
    groups = shards // members
    items, width = item_rows.shape
    features = basket_gain.shape[0]
    tiles, words, _ = tile_bits.shape
    half = BLOCK // 2
    item_half = items // 2
    hidden = 2 * gate_basket.shape[1]
    per = members * half
    core = lax.axis_index("mp")
    place = lax.axis_index("shard") % groups
    core_arr = core.astype(jnp.int32).reshape(1)

    def swap(x):
        return lax.ppermute(x, "mp", [(0, 1), (1, 0)])

    def gather(x):
        return [
            lax.ppermute(
                x, "shard", [(s, (((s // groups) ^ k) * groups) + s % groups) for s in range(shards)]
            )
            for k in range(1, members)
        ]

    def exchange(xs):
        return [
            lax.ppermute(
                xs[k - 1],
                "shard",
                [(s, (s // groups) * groups + ((s % groups) ^ k)) for s in range(shards)],
            )
            for k in range(1, groups)
        ]

    meta = jnp.stack([tile_dest % 128, tile_dest // 128, tile_item]).astype(BF16)
    meta = jnp.pad(meta, ((0, 13), (0, width - tiles)))
    pack = run(
        functools.partial(pack_body, half=half),
        sds((items + 2 * half + 16, width), BF16),
        (core_arr,),
        (item_rows, tile_bits.reshape(tiles * words, BLOCK), meta),
        scratch=[pltpu.VMEM((BLOCK, tiles * words), F32)] * 2,
        name="pack",
    )
    packs = [pack] + gather(pack)
    rows_other = swap(jnp.concatenate([q[:items] for q in packs], axis=0))
    cot_other = swap(lax.dynamic_slice_in_dim(item_cot, (1 - core) * item_half, item_half, 0))
    cot_mine = lax.dynamic_slice_in_dim(item_cot, core * item_half, item_half, 0)
    gate_b, up_b, down_b = gate_basket, up_basket, down_basket
    gate_bo, up_bo, down_bo = swap(gate_basket), swap(up_basket), swap(down_basket)
    gate_io, up_io, down_io = swap(gate_item), swap(up_item), swap(down_item)

    metas = jnp.stack([q[items + 2 * half : items + 2 * half + 3, :tiles] for q in packs])
    metas = metas.astype(jnp.int32)
    dest = metas[:, 0] + 128 * metas[:, 1]
    row_at = (((dest % groups) ^ place) * members + dest // groups) * half
    lane_at = metas[:, 2] * BLOCK + items * jnp.arange(members, dtype=jnp.int32)[:, None]
    idx = jnp.concatenate([jnp.stack([row_at, lane_at], axis=-1).reshape(-1), core_arr])

    source = lax.broadcasted_iota(jnp.int32, (2 * tiles * words, tiles * BLOCK), 0)
    target = lax.broadcasted_iota(jnp.int32, (2 * tiles * words, tiles * BLOCK), 1)
    spread = (
        (source % (tiles * words) == target // 16) & (source // (tiles * words) == (target // 8) % 2)
    ).astype(BF16)

    part_shapes = [sds((per, features), F32)] + [sds((per, features), BF16)] * (groups - 1)
    mt, *parts = run(
        functools.partial(
            sums_body, members=members, groups=groups, half=half, items=items, tiles=tiles
        ),
        [sds((shards * half, members * items), BF16)] + part_shapes,
        (idx,),
        (*packs, rows_other, spread),
        scratch=[pltpu.VMEM((members * items, features), BF16)],
        flops=1 << 30,
        name="sums",
    )
    received = exchange(parts[1:])
    mo = run(
        functools.partial(turn_body, items=items),
        sds((items, shards * half), BF16),
        (),
        (mt,),
        flops=1 << 29,
        name="turn",
    )
    item_hidden = run(
        item_hidden_body,
        sds((item_half, hidden), F32),
        (core_arr,),
        (cot_mine, cot_other, down_item, down_io),
        scratch=[pltpu.VMEM((item_half, features), BF16)],
        flops=1 << 29,
        name="item_hidden",
    )
    basket_out, basket_sum, value, slope = run(
        functools.partial(basket_body, groups=groups),
        [
            sds((per, features), BF16),
            sds((per, features), F32),
            sds((per, hidden), BF16),
            sds((per, hidden), BF16),
        ],
        (),
        (
            parts[0],
            *received,
            basket_gain.reshape(1, features),
            gate_b,
            gate_bo,
            up_b,
            up_bo,
            down_b,
            down_bo,
        ),
        flops=1 << 30,
        name="basket",
    )
    outs = [basket_out] + exchange([basket_out] * (groups - 1))
    message_mine, message_theirs = run(
        functools.partial(message_body, groups=groups),
        [sds((item_half, features), F32)] * 2,
        (core_arr,),
        (mo, *outs),
        scratch=[pltpu.VMEM((items, features), F32)],
        flops=1 << 28,
        name="message",
    )
    message_other = swap(message_theirs)
    grad_message = run(
        item_body,
        sds((item_half, features), BF16),
        (),
        (
            message_mine,
            message_other,
            item_hidden,
            item_gain.reshape(1, features),
            gate_item,
            gate_io,
            up_item,
            up_io,
        ),
        flops=1 << 30,
        name="item",
    )
    grads = [grad_message] + gather(grad_message)
    grads_other = swap(jnp.concatenate(grads, axis=0))
    grad_parts = run(
        functools.partial(grad_sums_body, members=members, groups=groups),
        part_shapes,
        (core_arr,),
        (mt, *grads, grads_other),
        scratch=[pltpu.VMEM((members * items, features), BF16)],
        flops=1 << 29,
        name="grad_sums",
    )
    grad_received = exchange(grad_parts[1:])
    grad_sum = run(
        functools.partial(basket_back_body, groups=groups),
        sds((per, features), BF16),
        (),
        (
            grad_parts[0],
            *grad_received,
            basket_sum,
            value,
            slope,
            basket_gain.reshape(1, features),
            gate_b,
            gate_bo,
            up_b,
            up_bo,
            down_b,
            down_bo,
        ),
        flops=1 << 30,
        name="basket_back",
    )
    sums = [grad_sum] + exchange([grad_sum] * (groups - 1))
    back_mine, back_theirs = run(
        functools.partial(back_body, groups=groups),
        [sds((items, width), F32)] * 2,
        (core_arr,),
        (mo, *sums),
        scratch=[pltpu.VMEM((items, features), F32)],
        flops=1 << 28,
        name="back",
    )
    back_other = swap(back_theirs)
    new_rows, new_first, new_second = run(
        adam_body,
        [sds((items, width), F32)] * 3,
        (),
        (back_mine, back_other, item_cot, item_rows, first_moment, second_moment),
        name="adam",
    )
    return (new_rows, new_first, new_second)


def solution(mesh):
    return jax.shard_map(
        local,
        mesh=mesh,
        in_specs=(
            P("shard", "mp"),
            P("shard", "mp"),
            P("shard", "mp"),
            P("shard", "mp"),
            P("shard", None, None),
            P("shard"),
            P("shard"),
            P(),
            P(),
            P(None, "mp"),
            P(None, "mp"),
            P("mp", None),
            P(None, "mp"),
            P(None, "mp"),
            P("mp", None),
        ),
        out_specs=(P("shard", "mp"), P("shard", "mp"), P("shard", "mp")),
        check_vma=False,
    )
```

```python
import functools

import jax
import jax.numpy as jnp
import numpy as np
from jax import lax
from jax.experimental import pallas as pl
from jax.experimental.pallas import tpu as pltpu
from jax.sharding import PartitionSpec as P

BLOCK = 128
GATHER = 4
CHUNK = 256

NORM_EPSILON = 1e-05
LEARNING_RATE = 0.01
BETA_FIRST = 0.9
BETA_SECOND = 0.99
ADAM_EPSILON = 1e-08


F32 = jnp.float32
BF16 = jnp.bfloat16


def sds(shape, dtype):
    return jax.ShapeDtypeStruct(shape, dtype)


def nbytes(x):
    return int(np.prod(x.shape)) * jnp.dtype(x.dtype).itemsize


def run(body, outs, smem, args, scratch=(), flops=1 << 20, name=None):
    limit = sum(nbytes(x) for x in (*args, *jax.tree.leaves(outs), *scratch)) + (4 << 20)
    specs = [pl.BlockSpec(memory_space=pltpu.SMEM)] * len(smem)
    specs += [pl.BlockSpec(memory_space=pltpu.VMEM)] * len(args)
    return pl.pallas_call(
        body,
        out_shape=outs,
        in_specs=specs,
        out_specs=jax.tree.map(lambda _: pl.BlockSpec(memory_space=pltpu.VMEM), outs),
        scratch_shapes=list(scratch),
        cost_estimate=pl.CostEstimate(flops=flops, bytes_accessed=1 << 20, transcendentals=0),
        compiler_params=pltpu.CompilerParams(vmem_limit_bytes=min(limit, 60 * 1024 * 1024)),
        name=name,
    )(*smem, *args)


def dot(a, b):
    return jnp.dot(a, b, preferred_element_type=F32)


def dot_nt(a, b):
    return lax.dot_general(a, b, (((1,), (1,)), ((), ())), preferred_element_type=F32)


def sigmoid(v):
    return 0.5 * jnp.tanh(0.5 * v) + 0.5


def pack_body(
    dest_ref, item_ref, rows_ref, words_ref, cot_ref, pack_ref, send_ref, lo_ref, hi_ref, *, half, members, groups
):
    items = rows_ref.shape[0]
    tiles = dest_ref.shape[0]
    core = lax.axis_index("mp")
    place = lax.axis_index("shard") % groups
    start = pl.multiple_of(core * half, half)
    pack_ref[0:items, :] = rows_ref[...].astype(BF16)
    words = words_ref[...]
    lo_ref[...] = (words & 255).astype(F32).T
    hi_ref[...] = (words >> 8).astype(F32).T
    pack_ref[items : items + half, :] = lo_ref[pl.ds(start, half), :].astype(BF16)
    pack_ref[items + half : items + 2 * half, :] = hi_ref[pl.ds(start, half), :].astype(BF16)
    lanes = lax.broadcasted_iota(jnp.int32, (16, pack_ref.shape[1]), 1)
    meta = jnp.zeros_like(lanes)
    for t in range(tiles):
        dest = dest_ref[t]
        slot = ((dest % groups) ^ place) * members + dest // groups
        meta = jnp.where(lanes == t, slot, meta)
        meta = jnp.where(lanes == tiles + t, item_ref[t], meta)
    pack_ref[items + 2 * half :, :] = meta.astype(F32).astype(BF16)
    rows = send_ref.shape[0]
    send_ref[...] = cot_ref[pl.ds(pl.multiple_of((1 - core) * rows, rows), rows), :]


def spread_body(pack_ref, out_ref):
    source = lax.broadcasted_iota(jnp.int32, (out_ref.shape[0], 2 * BLOCK), 0)
    words = out_ref.shape[0] // 2
    for c in range(0, out_ref.shape[1], 2 * BLOCK):
        target = lax.broadcasted_iota(jnp.int32, (out_ref.shape[0], 2 * BLOCK), 1) + c
        hit = source == (target // 16) + words * ((target // 8) % 2)
        out_ref[:, c : c + 2 * BLOCK] = jnp.where(hit, 1.0, 0.0).astype(BF16)


def join_halves(core, whole_ref, own_ref_list, other_ref, rows):
    width = other_ref.shape[1]
    mine = pl.multiple_of(core * width, width)
    theirs = pl.multiple_of((1 - core) * width, width)
    for l, own in enumerate(own_ref_list):
        whole_ref[l * rows : (l + 1) * rows, pl.ds(mine, width)] = own[0:rows, :]
        whole_ref[l * rows : (l + 1) * rows, pl.ds(theirs, width)] = other_ref[
            l * rows : (l + 1) * rows, :
        ]


def sums_body(idx_ref, *refs, members, groups, half, items, tiles):
    packs = refs[:members]
    other_ref, spread_ref = refs[members : members + 2]
    mt_ref = refs[members + 2]
    out_refs = refs[members + 3 : members + 3 + groups]
    rows_ref = refs[members + 3 + groups]
    core = lax.axis_index("mp")
    mt_ref[...] = jnp.zeros_like(mt_ref)
    byte_rows = jnp.concatenate(
        [
            jnp.concatenate(
                [p[items : items + half, :], p[items + half : items + 2 * half, :]], axis=1
            )
            for p in packs
        ],
        axis=0,
    )
    shift = lax.broadcasted_iota(jnp.int32, (members * half, 2 * BLOCK), 1) % 8
    for q in range(tiles // 2):
        spread = dot(byte_rows, spread_ref[:, q * 2 * BLOCK : (q + 1) * 2 * BLOCK])
        bits = jnp.right_shift(spread.astype(jnp.int32), shift) & 1
        mask = bits.astype(F32).astype(BF16)
        for l in range(members):
            for b in range(2):
                t = 2 * q + b
                row = pl.multiple_of(idx_ref[l, t] * half, half)
                lane = pl.multiple_of(idx_ref[l, tiles + t] * BLOCK + l * items, BLOCK)
                where = (pl.ds(row, half), pl.ds(lane, BLOCK))
                mt_ref[where] = (
                    mt_ref[where]
                    + mask[l * half : (l + 1) * half, b * BLOCK : (b + 1) * BLOCK]
                )
    join_halves(core, rows_ref, packs, other_ref, items)
    per = members * half
    for i in range(groups):
        total = dot(mt_ref[i * per : (i + 1) * per, :], rows_ref[...])
        out_refs[i][...] = total.astype(out_refs[i].dtype)


def turn_body(mt_ref, mine_ref, other_ref, down_a, down_b, out_ref, hid_ref, cot_ref, *, items):
    core = lax.axis_index("mp")
    width = mine_ref.shape[1]
    rows = other_ref.shape[0]
    cot_ref[:, pl.ds(pl.multiple_of(core * width, width), width)] = mine_ref[
        pl.ds(pl.multiple_of(core * rows, rows), rows), :
    ]
    cot_ref[:, pl.ds(pl.multiple_of((1 - core) * width, width), width)] = other_ref[...]
    cot = cot_ref[...]
    at = 0
    for down in (down_a, down_b):
        for c in range(0, down.shape[0], CHUNK):
            hid_ref[:, at : at + CHUNK] = dot_nt(cot, down[c : c + CHUNK, :])
            at += CHUNK
    for c in range(mt_ref.shape[0] // BLOCK):
        block = mt_ref[c * BLOCK : (c + 1) * BLOCK, 0:items].astype(F32)
        out_ref[:, c * BLOCK : (c + 1) * BLOCK] = block.T.astype(BF16)


def add_all(refs):
    total = refs[0][...].astype(F32)
    for r in refs[1:]:
        total = total + r[...].astype(F32)
    return total


def rms(values):
    return lax.rsqrt(jnp.mean(values * values, axis=-1, keepdims=True) + NORM_EPSILON)


def basket_body(*refs, groups):
    parts = refs[:groups]
    gain_ref, gate_a, gate_b, up_a, up_b, down_a, down_b = refs[groups : groups + 7]
    out_ref, sum_ref, value_ref, slope_ref = refs[groups + 7 :]
    total = add_all(parts)
    sum_ref[...] = total
    normed = total * rms(total) * gain_ref[...]
    normed_bf = normed.astype(BF16)
    acc = normed
    at = 0
    for gate, up, down in ((gate_a, up_a, down_a), (gate_b, up_b, down_b)):
        for c in range(0, gate.shape[1], CHUNK):
            gate_pre = dot(normed_bf, gate[:, c : c + CHUNK])
            up_pre = dot(normed_bf, up[:, c : c + CHUNK])
            sig = sigmoid(gate_pre)
            value = gate_pre * sig
            acc = acc + dot((value * up_pre).astype(BF16), down[c : c + CHUNK, :])
            value_ref[:, at : at + CHUNK] = value.astype(BF16)
            slope_ref[:, at : at + CHUNK] = (up_pre * (sig + value * (1.0 - sig))).astype(BF16)
            at += CHUNK
    out_ref[...] = acc.astype(BF16)


def message_body(mo_ref, *refs, groups):
    parts = refs[:groups]
    mine_ref, theirs_ref, all_ref = refs[groups:]
    per = parts[0].shape[0]
    total = dot(mo_ref[:, 0:per], parts[0][...])
    for i in range(1, groups):
        total = total + dot(mo_ref[:, i * per : (i + 1) * per], parts[i][...])
    all_ref[...] = total
    rows = mine_ref.shape[0]
    core = lax.axis_index("mp")
    mine_ref[...] = all_ref[pl.ds(pl.multiple_of(core * rows, rows), rows), :]
    theirs_ref[...] = all_ref[pl.ds(pl.multiple_of((1 - core) * rows, rows), rows), :]


def item_body(mine_ref, other_ref, hidden_ref, gain_ref, gate_a, gate_b, up_a, up_b, out_ref):
    message = mine_ref[...] + other_ref[...]
    scale = rms(message)
    gain = gain_ref[...]
    query = (message * scale * gain).astype(BF16)
    acc = jnp.zeros_like(message)
    at = 0
    for gate, up in ((gate_a, up_a), (gate_b, up_b)):
        for c in range(0, gate.shape[1], CHUNK):
            gate_w = gate[:, c : c + CHUNK]
            up_w = up[:, c : c + CHUNK]
            gate_pre = dot(query, gate_w)
            up_pre = dot(query, up_w)
            sig = sigmoid(gate_pre)
            value = gate_pre * sig
            hidden = hidden_ref[:, at : at + CHUNK]
            grad_up = (hidden * value).astype(BF16)
            grad_gate = (hidden * up_pre * (sig + value * (1.0 - sig))).astype(BF16)
            acc = acc + dot_nt(grad_gate, gate_w) + dot_nt(grad_up, up_w)
            at += CHUNK
    weighted = gain * acc
    inner = jnp.mean(weighted * message, axis=1, keepdims=True)
    cubed = scale * scale * scale
    out_ref[...] = (scale * weighted - message * (cubed * inner)).astype(BF16)


def grad_sums_body(mt_ref, *refs, members, groups):
    owns = refs[:members]
    other_ref = refs[members]
    out_refs = refs[members + 1 : members + 1 + groups]
    rows_ref = refs[members + 1 + groups]
    core = lax.axis_index("mp")
    rows = owns[0].shape[0]
    for l in range(members):
        mine = pl.multiple_of((2 * l + core) * rows, rows)
        theirs = pl.multiple_of((2 * l + 1 - core) * rows, rows)
        rows_ref[pl.ds(mine, rows), :] = owns[l][...]
        rows_ref[pl.ds(theirs, rows), :] = other_ref[l * rows : (l + 1) * rows, :]
    per = out_refs[0].shape[0]
    for i in range(groups):
        total = dot(mt_ref[i * per : (i + 1) * per, :], rows_ref[...])
        out_refs[i][...] = total.astype(out_refs[i].dtype)


def basket_back_body(*refs, groups):
    parts = refs[:groups]
    sum_ref, value_ref, slope_ref, gain_ref = refs[groups : groups + 4]
    gate_a, gate_b, up_a, up_b, down_a, down_b, out_ref = refs[groups + 4 :]
    grad_out = add_all(parts)
    grad_bf = grad_out.astype(BF16)
    acc = grad_out
    at = 0
    for gate, up, down in ((gate_a, up_a, down_a), (gate_b, up_b, down_b)):
        for c in range(0, gate.shape[1], CHUNK):
            hidden = dot_nt(grad_bf, down[c : c + CHUNK, :])
            grad_up = (hidden * value_ref[:, at : at + CHUNK].astype(F32)).astype(BF16)
            grad_gate = (hidden * slope_ref[:, at : at + CHUNK].astype(F32)).astype(BF16)
            acc = acc + dot_nt(grad_gate, gate[:, c : c + CHUNK])
            acc = acc + dot_nt(grad_up, up[:, c : c + CHUNK])
            at += CHUNK
    total = sum_ref[...]
    scale = rms(total)
    weighted = gain_ref[...] * acc
    inner = jnp.mean(weighted * total, axis=1, keepdims=True)
    cubed = scale * scale * scale
    out_ref[...] = (scale * weighted - total * (cubed * inner)).astype(BF16)


def back_body(mo_ref, *refs, groups):
    parts = refs[:groups]
    mine_ref, theirs_ref, all_ref = refs[groups:]
    per = parts[0].shape[0]
    total = dot(mo_ref[:, 0:per], parts[0][...])
    for i in range(1, groups):
        total = total + dot(mo_ref[:, i * per : (i + 1) * per], parts[i][...])
    all_ref[...] = total
    width = mine_ref.shape[1]
    core = lax.axis_index("mp")
    mine_ref[...] = all_ref[:, pl.ds(pl.multiple_of(core * width, width), width)]
    theirs_ref[...] = all_ref[:, pl.ds(pl.multiple_of((1 - core) * width, width), width)]


def adam_body(back_ref, other_ref, cot_ref, rows_ref, first_ref, second_ref, r_ref, f_ref, s_ref):
    gradient = cot_ref[...].astype(F32) + (back_ref[...] + other_ref[...])
    first = BETA_FIRST * first_ref[...] + (1.0 - BETA_FIRST) * gradient
    second = BETA_SECOND * second_ref[...] + (1.0 - BETA_SECOND) * gradient * gradient
    f_ref[...] = first
    s_ref[...] = second
    r_ref[...] = rows_ref[...] - LEARNING_RATE * first / (jnp.sqrt(second) + ADAM_EPSILON)


def local(
    item_rows,
    first_moment,
    second_moment,
    item_cot,
    tile_bits,
    tile_item,
    tile_dest,
    basket_gain,
    item_gain,
    gate_basket,
    up_basket,
    down_basket,
    gate_item,
    up_item,
    down_item,
):
    shards = lax.axis_size("shard")
    members = GATHER if shards % GATHER == 0 else 1
    groups = shards // members
    items, width = item_rows.shape
    features = basket_gain.shape[0]
    tiles, words, _ = tile_bits.shape
    half = BLOCK // 2
    item_half = items // 2
    hidden = 2 * gate_basket.shape[1]
    per = members * half
    def swap(x):
        return lax.ppermute(x, "mp", [(0, 1), (1, 0)])

    def gather(x):
        return [
            lax.ppermute(
                x, "shard", [(s, (((s // groups) ^ k) * groups) + s % groups) for s in range(shards)]
            )
            for k in range(1, members)
        ]

    def exchange(xs):
        return [
            lax.ppermute(
                xs[k - 1],
                "shard",
                [(s, (s // groups) * groups + ((s % groups) ^ k)) for s in range(shards)],
            )
            for k in range(1, groups)
        ]

    pack, cot_send = run(
        functools.partial(pack_body, half=half, members=members, groups=groups),
        [sds((items + 2 * half + 16, width), BF16), sds((item_half, width), BF16)],
        (tile_dest, tile_item),
        (item_rows, tile_bits.reshape(tiles * words, BLOCK), item_cot),
        scratch=[pltpu.VMEM((BLOCK, tiles * words), F32)] * 2,
        name="pack",
    )
    packs = [pack] + gather(pack)
    spread = run(
        spread_body,
        sds((2 * tiles * words, tiles * BLOCK), BF16),
        (),
        (pack,),
        flops=1 << 29,
        name="spread",
    )
    cot_other = swap(cot_send)
    gate_b, up_b, down_b = gate_basket, up_basket, down_basket
    gate_bo, up_bo, down_bo = swap(gate_basket), swap(up_basket), swap(down_basket)
    gate_io, up_io, down_io = swap(gate_item), swap(up_item), swap(down_item)
    rows_other = swap(jnp.concatenate([q[:items] for q in packs], axis=0))
    metas = [q[items + 2 * half : items + 2 * half + 1] for q in packs]
    idx = jnp.concatenate(metas, axis=0).astype(jnp.int32)

    part_shapes = [sds((per, features), F32)] + [sds((per, features), BF16)] * (groups - 1)
    mt, *parts = run(
        functools.partial(
            sums_body, members=members, groups=groups, half=half, items=items, tiles=tiles
        ),
        [sds((shards * half, members * items), BF16)] + part_shapes,
        (idx,),
        (*packs, rows_other, spread),
        scratch=[pltpu.VMEM((members * items, features), BF16)],
        flops=1 << 30,
        name="sums",
    )
    received = exchange(parts[1:])
    mo, item_hidden = run(
        functools.partial(turn_body, items=items),
        [sds((items, shards * half), BF16), sds((item_half, hidden), F32)],
        (),
        (mt, item_cot, cot_other, down_item, down_io),
        scratch=[pltpu.VMEM((item_half, features), BF16)],
        flops=1 << 29,
        name="turn",
    )
    basket_out, basket_sum, value, slope = run(
        functools.partial(basket_body, groups=groups),
        [
            sds((per, features), BF16),
            sds((per, features), F32),
            sds((per, hidden), BF16),
            sds((per, hidden), BF16),
        ],
        (),
        (
            parts[0],
            *received,
            basket_gain.reshape(1, features),
            gate_b,
            gate_bo,
            up_b,
            up_bo,
            down_b,
            down_bo,
        ),
        flops=1 << 30,
        name="basket",
    )
    outs = [basket_out] + exchange([basket_out] * (groups - 1))
    message_mine, message_theirs = run(
        functools.partial(message_body, groups=groups),
        [sds((item_half, features), F32)] * 2,
        (),
        (mo, *outs),
        scratch=[pltpu.VMEM((items, features), F32)],
        flops=1 << 28,
        name="message",
    )
    message_other = swap(message_theirs)
    grad_message = run(
        item_body,
        sds((item_half, features), BF16),
        (),
        (
            message_mine,
            message_other,
            item_hidden,
            item_gain.reshape(1, features),
            gate_item,
            gate_io,
            up_item,
            up_io,
        ),
        flops=1 << 30,
        name="item",
    )
    grads = [grad_message] + gather(grad_message)
    grads_other = swap(jnp.concatenate(grads, axis=0))
    grad_parts = run(
        functools.partial(grad_sums_body, members=members, groups=groups),
        part_shapes,
        (),
        (mt, *grads, grads_other),
        scratch=[pltpu.VMEM((members * items, features), BF16)],
        flops=1 << 29,
        name="grad_sums",
    )
    grad_received = exchange(grad_parts[1:])
    grad_sum = run(
        functools.partial(basket_back_body, groups=groups),
        sds((per, features), BF16),
        (),
        (
            grad_parts[0],
            *grad_received,
            basket_sum,
            value,
            slope,
            basket_gain.reshape(1, features),
            gate_b,
            gate_bo,
            up_b,
            up_bo,
            down_b,
            down_bo,
        ),
        flops=1 << 30,
        name="basket_back",
    )
    sums = [grad_sum] + exchange([grad_sum] * (groups - 1))
    back_mine, back_theirs = run(
        functools.partial(back_body, groups=groups),
        [sds((items, width), F32)] * 2,
        (),
        (mo, *sums),
        scratch=[pltpu.VMEM((items, features), F32)],
        flops=1 << 28,
        name="back",
    )
    back_other = swap(back_theirs)
    new_rows, new_first, new_second = run(
        adam_body,
        [sds((items, width), F32)] * 3,
        (),
        (back_mine, back_other, item_cot, item_rows, first_moment, second_moment),
        name="adam",
    )
    return (new_rows, new_first, new_second)


def solution(mesh):
    return jax.shard_map(
        local,
        mesh=mesh,
        in_specs=(
            P("shard", "mp"),
            P("shard", "mp"),
            P("shard", "mp"),
            P("shard", "mp"),
            P("shard", None, None),
            P("shard"),
            P("shard"),
            P(),
            P(),
            P(None, "mp"),
            P(None, "mp"),
            P("mp", None),
            P(None, "mp"),
            P(None, "mp"),
            P("mp", None),
        ),
        out_specs=(P("shard", "mp"), P("shard", "mp"), P("shard", "mp")),
        check_vma=False,
    )
```

```python
import functools

import jax
import jax.numpy as jnp
import numpy as np
from jax import lax
from jax.experimental import pallas as pl
from jax.experimental.pallas import tpu as pltpu
from jax.sharding import PartitionSpec as P


BLOCK = 128
GATHER = 4
CHUNK = 256

NORM_EPSILON = 1e-05
LEARNING_RATE = 0.01
BETA_FIRST = 0.9
BETA_SECOND = 0.99
ADAM_EPSILON = 1e-08


F32 = jnp.float32
BF16 = jnp.bfloat16


def sds(shape, dtype):
    return jax.ShapeDtypeStruct(shape, dtype)


def nbytes(x):
    return int(np.prod(x.shape)) * jnp.dtype(x.dtype).itemsize


def run(body, outs, smem, args, scratch=(), flops=1 << 20, far=(), limit=0):
    held = [x for x in scratch if isinstance(x.dtype, np.dtype) or x.dtype in (F32, BF16)]
    limit = limit or sum(nbytes(x) for x in (*args, *jax.tree.leaves(outs), *held)) + (4 << 20)
    specs = [pl.BlockSpec(memory_space=pltpu.HBM)] * len(far)
    specs += [pl.BlockSpec(memory_space=pltpu.SMEM)] * len(smem)
    specs += [pl.BlockSpec(memory_space=pltpu.VMEM)] * len(args)
    call = pl.pallas_call(
        body,
        out_shape=outs,
        in_specs=specs,
        out_specs=jax.tree.map(lambda _: pl.BlockSpec(memory_space=pltpu.VMEM), outs),
        scratch_shapes=list(scratch),
        cost_estimate=pl.CostEstimate(flops=flops, bytes_accessed=1 << 20, transcendentals=0),
        compiler_params=pltpu.CompilerParams(vmem_limit_bytes=min(limit, 60 * 1024 * 1024)),
    )
    far = [pltpu.with_memory_space_constraint(x, pltpu.HBM) for x in far]
    return call(*far, *smem, *args)


def dot(a, b):
    return jnp.dot(a, b, preferred_element_type=F32)


def dot_nt(a, b):
    return lax.dot_general(a, b, (((1,), (1,)), ((), ())), preferred_element_type=F32)


def sigmoid(v):
    return 0.5 * jnp.tanh(0.5 * v) + 0.5


def pack_body(
    dest_hbm,
    item_hbm,
    words_hbm,
    rows_hbm,
    cot_hbm,
    pack_ref,
    send_ref,
    dest_ref,
    item_ref,
    words_ref,
    rows_ref,
    turned_ref,
    sems,
    *,
    half,
    members,
    groups,
):
    items = rows_ref.shape[0]
    tiles = dest_ref.shape[0]
    core = lax.axis_index("mp")
    place = lax.axis_index("shard") % groups
    start = pl.multiple_of(core * half, half)
    rows = send_ref.shape[0]
    theirs = pl.ds(pl.multiple_of((1 - core) * rows, rows), rows)
    copies = [
        pltpu.make_async_copy(src, dst, sems.at[i])
        for i, (src, dst) in enumerate(
            (
                (words_hbm, words_ref),
                (dest_hbm, dest_ref),
                (item_hbm, item_ref),
                (rows_hbm, rows_ref),
                (cot_hbm.at[theirs, :], send_ref),
            )
        )
    ]
    for copy in copies:
        copy.start()
    copies[0].wait()
    turned_ref[...] = words_ref[...].astype(F32).T
    words = turned_ref[pl.ds(start, half), :].astype(jnp.int32)
    pack_ref[items : items + half, :] = (words & 255).astype(F32).astype(BF16)
    pack_ref[items + half : items + 2 * half, :] = (words >> 8).astype(F32).astype(BF16)
    copies[1].wait()
    copies[2].wait()
    lanes = lax.broadcasted_iota(jnp.int32, (16, pack_ref.shape[1]), 1)
    meta = jnp.zeros_like(lanes)
    for t in range(tiles):
        dest = dest_ref[t]
        slot = ((dest % groups) ^ place) * members + dest // groups
        meta = jnp.where(lanes == t, slot, meta)
        meta = jnp.where(lanes == tiles + t, item_ref[t], meta)
    pack_ref[items + 2 * half :, :] = meta.astype(F32).astype(BF16)
    copies[3].wait()
    pack_ref[0:items, :] = rows_ref[...].astype(BF16)
    copies[4].wait()


def spread_body(pack_ref, out_ref):
    source = lax.broadcasted_iota(jnp.int32, (out_ref.shape[0], 2 * BLOCK), 0)
    words = out_ref.shape[0] // 2
    for c in range(0, out_ref.shape[1], 2 * BLOCK):
        target = lax.broadcasted_iota(jnp.int32, (out_ref.shape[0], 2 * BLOCK), 1) + c
        hit = source == (target // 16) + words * ((target // 8) % 2)
        out_ref[:, c : c + 2 * BLOCK] = jnp.where(hit, 1.0, 0.0).astype(BF16)


def join_halves(core, whole_ref, own_ref_list, other_ref, rows):
    width = other_ref.shape[1]
    mine = pl.multiple_of(core * width, width)
    theirs = pl.multiple_of((1 - core) * width, width)
    for l, own in enumerate(own_ref_list):
        whole_ref[l * rows : (l + 1) * rows, pl.ds(mine, width)] = own[0:rows, :]
        whole_ref[l * rows : (l + 1) * rows, pl.ds(theirs, width)] = other_ref[
            l * rows : (l + 1) * rows, :
        ]


def masks_body(idx_ref, *refs, members, half, items, tiles):
    packs = refs[:members]
    spread_ref, mt_ref = refs[members:]
    mt_ref[...] = jnp.zeros_like(mt_ref)
    byte_rows = jnp.concatenate(
        [
            jnp.concatenate(
                [p[items : items + half, :], p[items + half : items + 2 * half, :]], axis=1
            )
            for p in packs
        ],
        axis=0,
    )
    shift = lax.broadcasted_iota(jnp.int32, (members * half, 2 * BLOCK), 1) % 8
    for q in range(tiles // 2):
        spread = dot(byte_rows, spread_ref[:, q * 2 * BLOCK : (q + 1) * 2 * BLOCK])
        bits = jnp.right_shift(spread.astype(jnp.int32), shift) & 1
        mask = bits.astype(F32).astype(BF16)
        for l in range(members):
            for b in range(2):
                t = 2 * q + b
                row = pl.multiple_of(idx_ref[l, t] * half, half)
                lane = pl.multiple_of(idx_ref[l, tiles + t] * BLOCK + l * items, BLOCK)
                where = (pl.ds(row, half), pl.ds(lane, BLOCK))
                mt_ref[where] = (
                    mt_ref[where]
                    + mask[l * half : (l + 1) * half, b * BLOCK : (b + 1) * BLOCK]
                )


def sums_body(mt_ref, *refs, members, groups, items):
    packs = refs[:members]
    other_ref = refs[members]
    out_refs = refs[members + 1 : members + 1 + groups]
    rows_ref = refs[members + 1 + groups]
    join_halves(lax.axis_index("mp"), rows_ref, packs, other_ref, items)
    per = out_refs[0].shape[0]
    for i in range(groups):
        total = dot(mt_ref[i * per : (i + 1) * per, :], rows_ref[...])
        out_refs[i][...] = total.astype(out_refs[i].dtype)


def turn_body(mt_ref, out_ref, *, items):
    for c in range(mt_ref.shape[0] // BLOCK):
        block = mt_ref[c * BLOCK : (c + 1) * BLOCK, 0:items].astype(F32)
        out_ref[:, c * BLOCK : (c + 1) * BLOCK] = block.T.astype(BF16)


def item_hidden_body(mine_ref, other_ref, down_a, down_b, hid_ref, cot_ref):
    core = lax.axis_index("mp")
    width = mine_ref.shape[1]
    rows = other_ref.shape[0]
    cot_ref[:, pl.ds(pl.multiple_of(core * width, width), width)] = mine_ref[
        pl.ds(pl.multiple_of(core * rows, rows), rows), :
    ]
    cot_ref[:, pl.ds(pl.multiple_of((1 - core) * width, width), width)] = other_ref[...]
    cot = cot_ref[...]
    at = 0
    for down in (down_a, down_b):
        for c in range(0, down.shape[0], CHUNK):
            hid_ref[:, at : at + CHUNK] = dot_nt(cot, down[c : c + CHUNK, :])
            at += CHUNK


def add_all(refs):
    total = refs[0][...].astype(F32)
    for r in refs[1:]:
        total = total + r[...].astype(F32)
    return total


def rms(values):
    return lax.rsqrt(jnp.mean(values * values, axis=-1, keepdims=True) + NORM_EPSILON)


def basket_body(*refs, groups):
    parts = refs[:groups]
    gain_ref, gate_a, gate_b, up_a, up_b, down_a, down_b = refs[groups : groups + 7]
    out_ref, sum_ref, value_ref, slope_ref = refs[groups + 7 :]
    total = add_all(parts)
    sum_ref[...] = total
    normed = total * rms(total) * gain_ref[...]
    normed_bf = normed.astype(BF16)
    acc = normed
    at = 0
    for gate, up, down in ((gate_a, up_a, down_a), (gate_b, up_b, down_b)):
        for c in range(0, gate.shape[1], CHUNK):
            gate_pre = dot(normed_bf, gate[:, c : c + CHUNK])
            up_pre = dot(normed_bf, up[:, c : c + CHUNK])
            sig = sigmoid(gate_pre)
            value = gate_pre * sig
            acc = acc + dot((value * up_pre).astype(BF16), down[c : c + CHUNK, :])
            value_ref[:, at : at + CHUNK] = value.astype(BF16)
            slope_ref[:, at : at + CHUNK] = (up_pre * (sig + value * (1.0 - sig))).astype(BF16)
            at += CHUNK
    out_ref[...] = acc.astype(BF16)


def message_body(mo_ref, *refs, groups):
    parts = refs[:groups]
    mine_ref, theirs_ref, all_ref = refs[groups:]
    per = parts[0].shape[0]
    total = dot(mo_ref[:, 0:per], parts[0][...])
    for i in range(1, groups):
        total = total + dot(mo_ref[:, i * per : (i + 1) * per], parts[i][...])
    all_ref[...] = total
    rows = mine_ref.shape[0]
    core = lax.axis_index("mp")
    mine_ref[...] = all_ref[pl.ds(pl.multiple_of(core * rows, rows), rows), :]
    theirs_ref[...] = all_ref[pl.ds(pl.multiple_of((1 - core) * rows, rows), rows), :]


def item_body(mine_ref, other_ref, hidden_ref, gain_ref, gate_a, gate_b, up_a, up_b, out_ref):
    message = mine_ref[...] + other_ref[...]
    scale = rms(message)
    gain = gain_ref[...]
    query = (message * scale * gain).astype(BF16)
    acc = jnp.zeros_like(message)
    at = 0
    for gate, up in ((gate_a, up_a), (gate_b, up_b)):
        for c in range(0, gate.shape[1], CHUNK):
            gate_w = gate[:, c : c + CHUNK]
            up_w = up[:, c : c + CHUNK]
            gate_pre = dot(query, gate_w)
            up_pre = dot(query, up_w)
            sig = sigmoid(gate_pre)
            value = gate_pre * sig
            hidden = hidden_ref[:, at : at + CHUNK]
            grad_up = (hidden * value).astype(BF16)
            grad_gate = (hidden * up_pre * (sig + value * (1.0 - sig))).astype(BF16)
            acc = acc + dot_nt(grad_gate, gate_w) + dot_nt(grad_up, up_w)
            at += CHUNK
    weighted = gain * acc
    inner = jnp.mean(weighted * message, axis=1, keepdims=True)
    cubed = scale * scale * scale
    out_ref[...] = (scale * weighted - message * (cubed * inner)).astype(BF16)


def grad_sums_body(mt_ref, *refs, members, groups):
    owns = refs[:members]
    other_ref = refs[members]
    out_refs = refs[members + 1 : members + 1 + groups]
    rows_ref = refs[members + 1 + groups]
    core = lax.axis_index("mp")
    rows = owns[0].shape[0]
    for l in range(members):
        mine = pl.multiple_of((2 * l + core) * rows, rows)
        theirs = pl.multiple_of((2 * l + 1 - core) * rows, rows)
        rows_ref[pl.ds(mine, rows), :] = owns[l][...]
        rows_ref[pl.ds(theirs, rows), :] = other_ref[l * rows : (l + 1) * rows, :]
    per = out_refs[0].shape[0]
    for i in range(groups):
        total = dot(mt_ref[i * per : (i + 1) * per, :], rows_ref[...])
        out_refs[i][...] = total.astype(out_refs[i].dtype)


def basket_back_body(*refs, groups):
    parts = refs[:groups]
    sum_ref, value_ref, slope_ref, gain_ref = refs[groups : groups + 4]
    gate_a, gate_b, up_a, up_b, down_a, down_b, out_ref = refs[groups + 4 :]
    grad_out = add_all(parts)
    grad_bf = grad_out.astype(BF16)
    acc = grad_out
    at = 0
    for gate, up, down in ((gate_a, up_a, down_a), (gate_b, up_b, down_b)):
        for c in range(0, gate.shape[1], CHUNK):
            hidden = dot_nt(grad_bf, down[c : c + CHUNK, :])
            grad_up = (hidden * value_ref[:, at : at + CHUNK].astype(F32)).astype(BF16)
            grad_gate = (hidden * slope_ref[:, at : at + CHUNK].astype(F32)).astype(BF16)
            acc = acc + dot_nt(grad_gate, gate[:, c : c + CHUNK])
            acc = acc + dot_nt(grad_up, up[:, c : c + CHUNK])
            at += CHUNK
    total = sum_ref[...]
    scale = rms(total)
    weighted = gain_ref[...] * acc
    inner = jnp.mean(weighted * total, axis=1, keepdims=True)
    cubed = scale * scale * scale
    out_ref[...] = (scale * weighted - total * (cubed * inner)).astype(BF16)


def back_body(mo_ref, *refs, groups):
    parts = refs[:groups]
    mine_ref, theirs_ref, all_ref = refs[groups:]
    per = parts[0].shape[0]
    total = dot(mo_ref[:, 0:per], parts[0][...])
    for i in range(1, groups):
        total = total + dot(mo_ref[:, i * per : (i + 1) * per], parts[i][...])
    all_ref[...] = total
    width = mine_ref.shape[1]
    core = lax.axis_index("mp")
    mine_ref[...] = all_ref[:, pl.ds(pl.multiple_of(core * width, width), width)]
    theirs_ref[...] = all_ref[:, pl.ds(pl.multiple_of((1 - core) * width, width), width)]


def adam_body(back_ref, other_ref, cot_ref, rows_ref, first_ref, second_ref, r_ref, f_ref, s_ref):
    gradient = cot_ref[...].astype(F32) + (back_ref[...] + other_ref[...])
    first = BETA_FIRST * first_ref[...] + (1.0 - BETA_FIRST) * gradient
    second = BETA_SECOND * second_ref[...] + (1.0 - BETA_SECOND) * gradient * gradient
    f_ref[...] = first
    s_ref[...] = second
    r_ref[...] = rows_ref[...] - LEARNING_RATE * first / (jnp.sqrt(second) + ADAM_EPSILON)


def local(
    item_rows,
    first_moment,
    second_moment,
    item_cot,
    tile_bits,
    tile_item,
    tile_dest,
    basket_gain,
    item_gain,
    gate_basket,
    up_basket,
    down_basket,
    gate_item,
    up_item,
    down_item,
):
    shards = lax.axis_size("shard")
    members = GATHER if shards % GATHER == 0 else 1
    groups = shards // members
    items, width = item_rows.shape
    features = basket_gain.shape[0]
    tiles, words, _ = tile_bits.shape
    half = BLOCK // 2
    item_half = items // 2
    hidden = 2 * gate_basket.shape[1]
    per = members * half

    def swap(x):
        return lax.ppermute(x, "mp", [(0, 1), (1, 0)])

    def gather(x):
        got = []
        for k in range(1, members):
            pairs = [(s, ((s // groups) ^ k) * groups + s % groups) for s in range(shards)]
            got.append(lax.ppermute(x, "shard", pairs))
        return got

    def exchange(xs):
        got = []
        for k in range(1, groups):
            pairs = [(s, (s // groups) * groups + ((s % groups) ^ k)) for s in range(shards)]
            got.append(lax.ppermute(xs[k - 1], "shard", pairs))
        return got

    pack, cot_send = run(
        functools.partial(pack_body, half=half, members=members, groups=groups),
        [sds((items + 2 * half + 16, width), BF16), sds((item_half, width), BF16)],
        (),
        (),
        far=(tile_dest, tile_item, tile_bits.reshape(tiles * words, BLOCK), item_rows, item_cot),
        scratch=[
            pltpu.SMEM((tiles,), jnp.int32),
            pltpu.SMEM((tiles,), jnp.int32),
            pltpu.VMEM((tiles * words, BLOCK), jnp.int32),
            pltpu.VMEM((items, width), F32),
            pltpu.VMEM((BLOCK, tiles * words), F32),
            pltpu.SemaphoreType.DMA((5,)),
        ],
    )
    packs = [pack] + gather(pack)
    spread = run(
        spread_body, sds((2 * tiles * words, tiles * BLOCK), BF16), (), (pack,), flops=1 << 29
    )
    cot_other = swap(cot_send)
    gate_b, up_b, down_b = gate_basket, up_basket, down_basket
    gate_bo, up_bo, down_bo = swap(gate_basket), swap(up_basket), swap(down_basket)
    rows_other = swap(jnp.concatenate([q[:items] for q in packs], axis=0))
    metas = [q[items + 2 * half : items + 2 * half + 1] for q in packs]
    idx = jnp.concatenate(metas, axis=0).astype(jnp.int32)

    part_shapes = [sds((per, features), F32)] + [sds((per, features), BF16)] * (groups - 1)
    mt = run(
        functools.partial(masks_body, members=members, half=half, items=items, tiles=tiles),
        sds((shards * half, members * items), BF16),
        (idx,),
        (*packs, spread),
        flops=1 << 29,
    )
    parts = run(
        functools.partial(sums_body, members=members, groups=groups, items=items),
        part_shapes,
        (),
        (mt, *packs, rows_other),
        scratch=[pltpu.VMEM((members * items, features), BF16)],
        flops=1 << 29,
    )
    received = exchange(parts[1:])
    mo = run(
        functools.partial(turn_body, items=items),
        sds((items, shards * half), BF16),
        (),
        (mt,),
        flops=1 << 29,
    )
    gate_io, up_io, down_io = swap(gate_item), swap(up_item), swap(down_item)
    basket_out, basket_sum, value, slope = run(
        functools.partial(basket_body, groups=groups),
        [
            sds((per, features), BF16),
            sds((per, features), F32),
            sds((per, hidden), BF16),
            sds((per, hidden), BF16),
        ],
        (),
        (
            parts[0],
            *received,
            basket_gain.reshape(1, features),
            gate_b,
            gate_bo,
            up_b,
            up_bo,
            down_b,
            down_bo,
        ),
        flops=1 << 30,
    )
    outs = [basket_out] + exchange([basket_out] * (groups - 1))
    item_hidden = run(
        item_hidden_body,
        sds((item_half, hidden), F32),
        (),
        (item_cot, cot_other, down_item, down_io),
        scratch=[pltpu.VMEM((item_half, features), BF16)],
        flops=1 << 29,
    )
    message_mine, message_theirs = run(
        functools.partial(message_body, groups=groups),
        [sds((item_half, features), F32)] * 2,
        (),
        (mo, *outs),
        scratch=[pltpu.VMEM((items, features), F32)],
        flops=1 << 28,
    )
    message_other = swap(message_theirs)
    grad_message = run(
        item_body,
        sds((item_half, features), BF16),
        (),
        (
            message_mine,
            message_other,
            item_hidden,
            item_gain.reshape(1, features),
            gate_item,
            gate_io,
            up_item,
            up_io,
        ),
        flops=1 << 30,
    )
    grads = [grad_message] + gather(grad_message)
    grads_other = swap(jnp.concatenate(grads, axis=0))
    grad_parts = run(
        functools.partial(grad_sums_body, members=members, groups=groups),
        part_shapes,
        (),
        (mt, *grads, grads_other),
        scratch=[pltpu.VMEM((members * items, features), BF16)],
        flops=1 << 29,
    )
    grad_received = exchange(grad_parts[1:])
    grad_sum = run(
        functools.partial(basket_back_body, groups=groups),
        sds((per, features), BF16),
        (),
        (
            grad_parts[0],
            *grad_received,
            basket_sum,
            value,
            slope,
            basket_gain.reshape(1, features),
            gate_b,
            gate_bo,
            up_b,
            up_bo,
            down_b,
            down_bo,
        ),
        flops=1 << 30,
    )
    sums = [grad_sum] + exchange([grad_sum] * (groups - 1))
    back_mine, back_theirs = run(
        functools.partial(back_body, groups=groups),
        [sds((items, width), F32)] * 2,
        (),
        (mo, *sums),
        scratch=[pltpu.VMEM((items, features), F32)],
        flops=1 << 28,
    )
    back_other = swap(back_theirs)
    new_rows, new_first, new_second = run(
        adam_body,
        [sds((items, width), F32)] * 3,
        (),
        (back_mine, back_other, item_cot, item_rows, first_moment, second_moment),
    )
    return (new_rows, new_first, new_second)


def solution(mesh):
    return jax.shard_map(
        local,
        mesh=mesh,
        in_specs=(
            P("shard", "mp"),
            P("shard", "mp"),
            P("shard", "mp"),
            P("shard", "mp"),
            P("shard", None, None),
            P("shard"),
            P("shard"),
            P(),
            P(),
            P(None, "mp"),
            P(None, "mp"),
            P("mp", None),
            P(None, "mp"),
            P(None, "mp"),
            P("mp", None),
        ),
        out_specs=(P("shard", "mp"), P("shard", "mp"), P("shard", "mp")),
        check_vma=False,
    )
```

```python
import functools

import jax
import jax.numpy as jnp
import numpy as np
from jax import lax
from jax.experimental import pallas as pl
from jax.experimental.pallas import tpu as pltpu
from jax.sharding import PartitionSpec as P


BLOCK = 128
GATHER = 4
CHUNK = 256

NORM_EPSILON = 1e-05
LEARNING_RATE = 0.01
BETA_FIRST = 0.9
BETA_SECOND = 0.99
ADAM_EPSILON = 1e-08


F32 = jnp.float32
BF16 = jnp.bfloat16


def sds(shape, dtype):
    return jax.ShapeDtypeStruct(shape, dtype)


def nbytes(x):
    return int(np.prod(x.shape)) * jnp.dtype(x.dtype).itemsize


def run(body, outs, smem, args, scratch=(), flops=1 << 20, far=(), limit=0):
    held = [x for x in scratch if isinstance(x.dtype, np.dtype) or x.dtype in (F32, BF16)]
    limit = limit or sum(nbytes(x) for x in (*args, *jax.tree.leaves(outs), *held)) + (4 << 20)
    specs = [pl.BlockSpec(memory_space=pltpu.HBM)] * len(far)
    specs += [pl.BlockSpec(memory_space=pltpu.SMEM)] * len(smem)
    specs += [pl.BlockSpec(memory_space=pltpu.VMEM)] * len(args)
    call = pl.pallas_call(
        body,
        out_shape=outs,
        in_specs=specs,
        out_specs=jax.tree.map(lambda _: pl.BlockSpec(memory_space=pltpu.VMEM), outs),
        scratch_shapes=list(scratch),
        cost_estimate=pl.CostEstimate(flops=flops, bytes_accessed=1 << 20, transcendentals=0),
        compiler_params=pltpu.CompilerParams(vmem_limit_bytes=min(limit, 60 * 1024 * 1024)),
    )
    far = [pltpu.with_memory_space_constraint(x, pltpu.HBM) for x in far]
    return call(*far, *smem, *args)


def dot(a, b):
    return jnp.dot(a, b, preferred_element_type=F32)


def dot_nt(a, b):
    return lax.dot_general(a, b, (((1,), (1,)), ((), ())), preferred_element_type=F32)


def sigmoid(v):
    return 0.5 * jnp.tanh(0.5 * v) + 0.5


def pack_body(
    dest_hbm,
    item_hbm,
    words_hbm,
    rows_hbm,
    cot_hbm,
    pack_ref,
    inc_ref,
    send_ref,
    dest_ref,
    item_ref,
    words_ref,
    rows_ref,
    turned_ref,
    sems,
    *,
    half,
    members,
    groups,
):
    items = rows_ref.shape[0]
    tiles = dest_ref.shape[0]
    core = lax.axis_index("mp")
    place = lax.axis_index("shard") % groups
    start = pl.multiple_of(core * half, half)
    rows = send_ref.shape[0]
    theirs = pl.ds(pl.multiple_of((1 - core) * rows, rows), rows)
    copies = [
        pltpu.make_async_copy(src, dst, sems.at[i])
        for i, (src, dst) in enumerate(
            (
                (words_hbm, words_ref),
                (dest_hbm, dest_ref),
                (item_hbm, item_ref),
                (rows_hbm, rows_ref),
                (cot_hbm.at[theirs, :], send_ref),
            )
        )
    ]
    for copy in copies:
        copy.start()
    copies[0].wait()
    turned_ref[...] = words_ref[...].astype(F32).T
    words = turned_ref[pl.ds(start, half), :].astype(jnp.int32)
    pack_ref[items : items + half, :] = (words & 255).astype(F32).astype(BF16)
    pack_ref[items + half : items + 2 * half, :] = (words >> 8).astype(F32).astype(BF16)
    copies[1].wait()
    copies[2].wait()
    lanes = lax.broadcasted_iota(jnp.int32, (16, pack_ref.shape[1]), 1)
    meta = jnp.zeros_like(lanes)
    for t in range(tiles):
        dest = dest_ref[t]
        slot = ((dest % groups) ^ place) * members + dest // groups
        meta = jnp.where(lanes == t, slot, meta)
        meta = jnp.where(lanes == tiles + t, item_ref[t], meta)
    pack_ref[items + 2 * half :, :] = meta.astype(F32).astype(BF16)
    inc_ref[...] = pack_ref[items:, :]
    copies[3].wait()
    pack_ref[0:items, :] = rows_ref[...].astype(BF16)
    copies[4].wait()


def spread_body(pack_ref, out_ref):
    source = lax.broadcasted_iota(jnp.int32, (out_ref.shape[0], 2 * BLOCK), 0)
    words = out_ref.shape[0] // 2
    for c in range(0, out_ref.shape[1], 2 * BLOCK):
        target = lax.broadcasted_iota(jnp.int32, (out_ref.shape[0], 2 * BLOCK), 1) + c
        hit = source == (target // 16) + words * ((target // 8) % 2)
        out_ref[:, c : c + 2 * BLOCK] = jnp.where(hit, 1.0, 0.0).astype(BF16)


def join_halves(core, whole_ref, own_ref_list, other_ref, rows):
    width = other_ref.shape[1]
    mine = pl.multiple_of(core * width, width)
    theirs = pl.multiple_of((1 - core) * width, width)
    for l, own in enumerate(own_ref_list):
        whole_ref[l * rows : (l + 1) * rows, pl.ds(mine, width)] = own[0:rows, :]
        whole_ref[l * rows : (l + 1) * rows, pl.ds(theirs, width)] = other_ref[
            l * rows : (l + 1) * rows, :
        ]


def masks_body(idx_ref, *refs, per, half, items, tiles, own):
    incs = refs[:-2]
    spread_ref, mt_ref = refs[-2:]
    first = incs[0].shape[0] - 2 * half - 16
    mt_ref[...] = jnp.zeros_like(mt_ref)
    byte_rows = jnp.concatenate(
        [
            jnp.concatenate(
                [p[first : first + half, :], p[first + half : first + 2 * half, :]], axis=1
            )
            for p in incs
        ],
        axis=0,
    )
    shift = lax.broadcasted_iota(jnp.int32, (len(incs) * half, 2 * BLOCK), 1) % 8
    for q in range(tiles // 2):
        spread = dot(byte_rows, spread_ref[:, q * 2 * BLOCK : (q + 1) * 2 * BLOCK])
        bits = jnp.right_shift(spread.astype(jnp.int32), shift) & 1
        mask = bits.astype(F32).astype(BF16)
        for l in range(len(incs)):
            for b in range(2):
                t = 2 * q + b
                slot = idx_ref[l, t]
                if own:
                    slot = jnp.where(slot // per == l, slot % per, per)
                row = pl.multiple_of(slot * half, half)
                lane = pl.multiple_of(idx_ref[l, tiles + t] * BLOCK + l * items, BLOCK)
                where = (pl.ds(row, half), pl.ds(lane, BLOCK))
                mt_ref[where] = (
                    mt_ref[where]
                    + mask[l * half : (l + 1) * half, b * BLOCK : (b + 1) * BLOCK]
                )


def sums_body(mt_ref, *refs, members, groups, items):
    packs = refs[:members]
    other_ref = refs[members]
    out_refs = refs[members + 1 : members + 1 + groups]
    rows_ref = refs[members + 1 + groups]
    join_halves(lax.axis_index("mp"), rows_ref, packs, other_ref, items)
    per = out_refs[0].shape[0]
    for i in range(groups):
        total = dot(mt_ref[i * per : (i + 1) * per, :], rows_ref[...])
        out_refs[i][...] = total.astype(out_refs[i].dtype)


def turn_body(mt_ref, out_ref):
    for c in range(0, out_ref.shape[1], BLOCK):
        out_ref[:, c : c + BLOCK] = mt_ref[c : c + BLOCK, :].astype(F32).T.astype(BF16)


def item_hidden_body(mine_ref, other_ref, down_a, down_b, hid_ref, cot_ref):
    core = lax.axis_index("mp")
    width = mine_ref.shape[1]
    rows = other_ref.shape[0]
    cot_ref[:, pl.ds(pl.multiple_of(core * width, width), width)] = mine_ref[
        pl.ds(pl.multiple_of(core * rows, rows), rows), :
    ]
    cot_ref[:, pl.ds(pl.multiple_of((1 - core) * width, width), width)] = other_ref[...]
    cot = cot_ref[...]
    at = 0
    for down in (down_a, down_b):
        for c in range(0, down.shape[0], CHUNK):
            hid_ref[:, at : at + CHUNK] = dot_nt(cot, down[c : c + CHUNK, :])
            at += CHUNK


def add_all(refs):
    total = refs[0][...].astype(F32)
    for r in refs[1:]:
        total = total + r[...].astype(F32)
    return total


def rms(values):
    return lax.rsqrt(jnp.mean(values * values, axis=-1, keepdims=True) + NORM_EPSILON)


def basket_body(*refs, groups):
    parts = refs[:groups]
    gain_ref, gate_a, gate_b, up_a, up_b, down_a, down_b = refs[groups : groups + 7]
    out_ref, sum_ref, value_ref, slope_ref = refs[groups + 7 :]
    total = add_all(parts)
    sum_ref[...] = total
    normed = total * rms(total) * gain_ref[...]
    normed_bf = normed.astype(BF16)
    acc = normed
    at = 0
    for gate, up, down in ((gate_a, up_a, down_a), (gate_b, up_b, down_b)):
        for c in range(0, gate.shape[1], CHUNK):
            gate_pre = dot(normed_bf, gate[:, c : c + CHUNK])
            up_pre = dot(normed_bf, up[:, c : c + CHUNK])
            sig = sigmoid(gate_pre)
            value = gate_pre * sig
            acc = acc + dot((value * up_pre).astype(BF16), down[c : c + CHUNK, :])
            value_ref[:, at : at + CHUNK] = value.astype(BF16)
            slope_ref[:, at : at + CHUNK] = (up_pre * (sig + value * (1.0 - sig))).astype(BF16)
            at += CHUNK
    out_ref[...] = acc.astype(BF16)


def message_body(mo_ref, out_ref, mine_ref, theirs_ref, all_ref, *, peers):
    all_ref[...] = dot(mo_ref[...], out_ref[...])
    rows = mine_ref.shape[0] // peers
    core = lax.axis_index("mp")
    for l in range(peers):
        mine = pl.multiple_of((2 * l + core) * rows, rows)
        theirs = pl.multiple_of((2 * l + 1 - core) * rows, rows)
        mine_ref[l * rows : (l + 1) * rows, :] = all_ref[pl.ds(mine, rows), :]
        theirs_ref[l * rows : (l + 1) * rows, :] = all_ref[pl.ds(theirs, rows), :].astype(BF16)


def join_body(mine_ref, other_ref, *out_refs):
    rows = out_refs[0].shape[0]
    for l, out in enumerate(out_refs):
        at = slice(l * rows, (l + 1) * rows)
        out[...] = (mine_ref[at, :] + other_ref[at, :].astype(F32)).astype(out.dtype)


def item_body(*refs, peers):
    hidden_ref, gain_ref, gate_a, gate_b, up_a, up_b, out_ref = refs[peers:]
    message = add_all(refs[:peers])
    scale = rms(message)
    gain = gain_ref[...]
    query = (message * scale * gain).astype(BF16)
    acc = jnp.zeros_like(message)
    at = 0
    for gate, up in ((gate_a, up_a), (gate_b, up_b)):
        for c in range(0, gate.shape[1], CHUNK):
            gate_w = gate[:, c : c + CHUNK]
            up_w = up[:, c : c + CHUNK]
            gate_pre = dot(query, gate_w)
            up_pre = dot(query, up_w)
            sig = sigmoid(gate_pre)
            value = gate_pre * sig
            hidden = hidden_ref[:, at : at + CHUNK]
            grad_up = (hidden * value).astype(BF16)
            grad_gate = (hidden * up_pre * (sig + value * (1.0 - sig))).astype(BF16)
            acc = acc + dot_nt(grad_gate, gate_w) + dot_nt(grad_up, up_w)
            at += CHUNK
    weighted = gain * acc
    inner = jnp.mean(weighted * message, axis=1, keepdims=True)
    cubed = scale * scale * scale
    out_ref[...] = (scale * weighted - message * (cubed * inner)).astype(BF16)


def grad_sums_body(mt_ref, *refs, members, groups):
    owns = refs[:members]
    other_ref = refs[members]
    out_refs = refs[members + 1 : members + 1 + groups]
    rows_ref = refs[members + 1 + groups]
    core = lax.axis_index("mp")
    rows = owns[0].shape[0]
    for l in range(members):
        mine = pl.multiple_of((2 * l + core) * rows, rows)
        theirs = pl.multiple_of((2 * l + 1 - core) * rows, rows)
        rows_ref[pl.ds(mine, rows), :] = owns[l][...]
        rows_ref[pl.ds(theirs, rows), :] = other_ref[l * rows : (l + 1) * rows, :]
    per = out_refs[0].shape[0]
    for i in range(groups):
        total = dot(mt_ref[i * per : (i + 1) * per, :], rows_ref[...])
        out_refs[i][...] = total.astype(out_refs[i].dtype)


def basket_back_body(*refs, groups):
    parts = refs[:groups]
    sum_ref, value_ref, slope_ref, gain_ref = refs[groups : groups + 4]
    gate_a, gate_b, up_a, up_b, down_a, down_b, out_ref = refs[groups + 4 :]
    grad_out = add_all(parts)
    grad_bf = grad_out.astype(BF16)
    acc = grad_out
    at = 0
    for gate, up, down in ((gate_a, up_a, down_a), (gate_b, up_b, down_b)):
        for c in range(0, gate.shape[1], CHUNK):
            hidden = dot_nt(grad_bf, down[c : c + CHUNK, :])
            grad_up = (hidden * value_ref[:, at : at + CHUNK].astype(F32)).astype(BF16)
            grad_gate = (hidden * slope_ref[:, at : at + CHUNK].astype(F32)).astype(BF16)
            acc = acc + dot_nt(grad_gate, gate[:, c : c + CHUNK])
            acc = acc + dot_nt(grad_up, up[:, c : c + CHUNK])
            at += CHUNK
    total = sum_ref[...]
    scale = rms(total)
    weighted = gain_ref[...] * acc
    inner = jnp.mean(weighted * total, axis=1, keepdims=True)
    cubed = scale * scale * scale
    out_ref[...] = (scale * weighted - total * (cubed * inner)).astype(BF16)


def back_body(mo_ref, sum_ref, mine_ref, theirs_ref, all_ref):
    all_ref[...] = dot(mo_ref[...], sum_ref[...])
    width = mine_ref.shape[1]
    core = lax.axis_index("mp")
    mine_ref[...] = all_ref[:, pl.ds(pl.multiple_of(core * width, width), width)]
    theirs = all_ref[:, pl.ds(pl.multiple_of((1 - core) * width, width), width)]
    theirs_ref[...] = theirs.astype(BF16)


def adam_body(*refs, peers):
    cot_ref, rows_ref, first_ref, second_ref, r_ref, f_ref, s_ref = refs[peers:]
    gradient = cot_ref[...].astype(F32) + add_all(refs[:peers])
    first = BETA_FIRST * first_ref[...] + (1.0 - BETA_FIRST) * gradient
    second = BETA_SECOND * second_ref[...] + (1.0 - BETA_SECOND) * gradient * gradient
    f_ref[...] = first
    s_ref[...] = second
    r_ref[...] = rows_ref[...] - LEARNING_RATE * first / (jnp.sqrt(second) + ADAM_EPSILON)


def local(
    item_rows,
    first_moment,
    second_moment,
    item_cot,
    tile_bits,
    tile_item,
    tile_dest,
    basket_gain,
    item_gain,
    gate_basket,
    up_basket,
    down_basket,
    gate_item,
    up_item,
    down_item,
):
    shards = lax.axis_size("shard")
    members = GATHER if shards % GATHER == 0 else 1
    groups = shards // members
    items, width = item_rows.shape
    features = basket_gain.shape[0]
    tiles, words, _ = tile_bits.shape
    half = BLOCK // 2
    item_half = items // 2
    hidden = 2 * gate_basket.shape[1]
    per = members * half

    def swap(x):
        return lax.ppermute(x, "mp", [(0, 1), (1, 0)])

    def gather(x):
        got = []
        for k in range(1, members):
            pairs = [(s, ((s // groups) ^ k) * groups + s % groups) for s in range(shards)]
            got.append(lax.ppermute(x, "shard", pairs))
        return got

    def exchange(xs):
        got = [xs[0]]
        for k in range(1, groups):
            pairs = [(s, (s // groups) * groups + ((s % groups) ^ k)) for s in range(shards)]
            got.append(lax.ppermute(xs[k], "shard", pairs))
        return got

    pack, inc, cot_send = run(
        functools.partial(pack_body, half=half, members=members, groups=groups),
        [
            sds((items + 2 * half + 16, width), BF16),
            sds((2 * half + 16, width), BF16),
            sds((item_half, width), BF16),
        ],
        (),
        (),
        far=(tile_dest, tile_item, tile_bits.reshape(tiles * words, BLOCK), item_rows, item_cot),
        scratch=[
            pltpu.SMEM((tiles,), jnp.int32),
            pltpu.SMEM((tiles,), jnp.int32),
            pltpu.VMEM((tiles * words, BLOCK), jnp.int32),
            pltpu.VMEM((items, width), F32),
            pltpu.VMEM((BLOCK, tiles * words), F32),
            pltpu.SemaphoreType.DMA((5,)),
        ],
    )
    packs = [pack] + gather(pack)
    spread = run(
        spread_body, sds((2 * tiles * words, tiles * BLOCK), BF16), (), (pack,), flops=1 << 29
    )
    cot_other = swap(cot_send)
    gate_b, up_b, down_b = gate_basket, up_basket, down_basket
    gate_bo, up_bo, down_bo = swap(gate_basket), swap(up_basket), swap(down_basket)
    rows_other = swap(jnp.concatenate([q[:items] for q in packs], axis=0))
    incs = exchange([inc] * groups)
    metas = [q[items + 2 * half : items + 2 * half + 1] for q in packs]
    idx = jnp.concatenate(metas, axis=0).astype(jnp.int32)
    metas = [q[2 * half : 2 * half + 1] for q in incs]
    idx_plane = jnp.concatenate(metas, axis=0).astype(jnp.int32)

    part_shapes = [sds((per, features), F32)] + [sds((per, features), BF16)] * (groups - 1)
    mt = run(
        functools.partial(
            masks_body, per=members, half=half, items=items, tiles=tiles, own=False
        ),
        sds((shards * half, members * items), BF16),
        (idx,),
        (*packs, spread),
        flops=1 << 29,
    )
    parts = run(
        functools.partial(sums_body, members=members, groups=groups, items=items),
        part_shapes,
        (),
        (mt, *packs, rows_other),
        scratch=[pltpu.VMEM((members * items, features), BF16)],
        flops=1 << 29,
    )
    received = exchange(parts)
    mt_plane = run(
        functools.partial(
            masks_body, per=members, half=half, items=items, tiles=tiles, own=True
        ),
        sds(((members + 1) * half, groups * items), BF16),
        (idx_plane,),
        (*incs, spread),
        flops=1 << 29,
    )
    mo = run(turn_body, sds((groups * items, per), BF16), (), (mt_plane,), flops=1 << 28)
    gate_io, up_io, down_io = swap(gate_item), swap(up_item), swap(down_item)
    basket_out, basket_sum, value, slope = run(
        functools.partial(basket_body, groups=groups),
        [
            sds((per, features), BF16),
            sds((per, features), F32),
            sds((per, hidden), BF16),
            sds((per, hidden), BF16),
        ],
        (),
        (
            *received,
            basket_gain.reshape(1, features),
            gate_b,
            gate_bo,
            up_b,
            up_bo,
            down_b,
            down_bo,
        ),
        flops=1 << 30,
    )
    message_mine, message_theirs = run(
        functools.partial(message_body, peers=groups),
        [sds((groups * item_half, features), F32), sds((groups * item_half, features), BF16)],
        (),
        (mo, basket_out),
        scratch=[pltpu.VMEM((groups * items, features), F32)],
        flops=1 << 28,
    )
    message_other = swap(message_theirs)
    item_hidden = run(
        item_hidden_body,
        sds((item_half, hidden), F32),
        (),
        (item_cot, cot_other, down_item, down_io),
        scratch=[pltpu.VMEM((item_half, features), BF16)],
        flops=1 << 29,
    )
    messages = run(
        join_body,
        [sds((item_half, features), F32)] + [sds((item_half, features), BF16)] * (groups - 1),
        (),
        (message_mine, message_other),
    )
    grad_message = run(
        functools.partial(item_body, peers=groups),
        sds((item_half, features), BF16),
        (),
        (
            *exchange(messages),
            item_hidden,
            item_gain.reshape(1, features),
            gate_item,
            gate_io,
            up_item,
            up_io,
        ),
        flops=1 << 30,
    )
    grads = [grad_message] + gather(grad_message)
    grads_other = swap(jnp.concatenate(grads, axis=0))
    grad_parts = run(
        functools.partial(grad_sums_body, members=members, groups=groups),
        part_shapes,
        (),
        (mt, *grads, grads_other),
        scratch=[pltpu.VMEM((members * items, features), BF16)],
        flops=1 << 29,
    )
    grad_received = exchange(grad_parts)
    grad_sum = run(
        functools.partial(basket_back_body, groups=groups),
        sds((per, features), BF16),
        (),
        (
            *grad_received,
            basket_sum,
            value,
            slope,
            basket_gain.reshape(1, features),
            gate_b,
            gate_bo,
            up_b,
            up_bo,
            down_b,
            down_bo,
        ),
        flops=1 << 30,
    )
    back_mine, back_theirs = run(
        back_body,
        [sds((groups * items, width), F32), sds((groups * items, width), BF16)],
        (),
        (mo, grad_sum),
        scratch=[pltpu.VMEM((groups * items, features), F32)],
        flops=1 << 28,
    )
    back_other = swap(back_theirs)
    backs = run(
        join_body,
        [sds((items, width), F32)] + [sds((items, width), BF16)] * (groups - 1),
        (),
        (back_mine, back_other),
    )
    new_rows, new_first, new_second = run(
        functools.partial(adam_body, peers=groups),
        [sds((items, width), F32)] * 3,
        (),
        (*exchange(backs), item_cot, item_rows, first_moment, second_moment),
    )
    return (new_rows, new_first, new_second)


def solution(mesh):
    return jax.shard_map(
        local,
        mesh=mesh,
        in_specs=(
            P("shard", "mp"),
            P("shard", "mp"),
            P("shard", "mp"),
            P("shard", "mp"),
            P("shard", None, None),
            P("shard"),
            P("shard"),
            P(),
            P(),
            P(None, "mp"),
            P(None, "mp"),
            P("mp", None),
            P(None, "mp"),
            P(None, "mp"),
            P("mp", None),
        ),
        out_specs=(P("shard", "mp"), P("shard", "mp"), P("shard", "mp")),
        check_vma=False,
    )
```

```python
import functools

import jax
import jax.numpy as jnp
import numpy as np
from jax import lax
from jax.experimental import pallas as pl
from jax.experimental.pallas import tpu as pltpu
from jax.sharding import PartitionSpec as P


BLOCK = 128
GATHER = 4
CHUNK = 1024

NORM_EPSILON = 1e-05
LEARNING_RATE = 0.01
BETA_FIRST = 0.9
BETA_SECOND = 0.99
ADAM_EPSILON = 1e-08


F32 = jnp.float32
BF16 = jnp.bfloat16


def sds(shape, dtype):
    return jax.ShapeDtypeStruct(shape, dtype)


def nbytes(x):
    return int(np.prod(x.shape)) * jnp.dtype(x.dtype).itemsize


def run(body, outs, smem, args, scratch=(), flops=1 << 20, far=(), limit=0):
    held = [x for x in scratch if isinstance(x.dtype, np.dtype) or x.dtype in (F32, BF16)]
    limit = limit or sum(nbytes(x) for x in (*args, *jax.tree.leaves(outs), *held)) + (4 << 20)
    specs = [pl.BlockSpec(memory_space=pltpu.HBM)] * len(far)
    specs += [pl.BlockSpec(memory_space=pltpu.SMEM)] * len(smem)
    specs += [pl.BlockSpec(memory_space=pltpu.VMEM)] * len(args)
    call = pl.pallas_call(
        body,
        out_shape=outs,
        in_specs=specs,
        out_specs=jax.tree.map(lambda _: pl.BlockSpec(memory_space=pltpu.VMEM), outs),
        scratch_shapes=list(scratch),
        cost_estimate=pl.CostEstimate(flops=flops, bytes_accessed=1 << 20, transcendentals=0),
        compiler_params=pltpu.CompilerParams(vmem_limit_bytes=min(limit, 60 * 1024 * 1024)),
    )
    far = [pltpu.with_memory_space_constraint(x, pltpu.HBM) for x in far]
    return call(*far, *smem, *args)


def dot(a, b):
    return jnp.dot(a, b, preferred_element_type=F32)


def dot_nt(a, b):
    return lax.dot_general(a, b, (((1,), (1,)), ((), ())), preferred_element_type=F32)


def sigmoid(v):
    return 0.5 * jnp.tanh(0.5 * v) + 0.5


def crossed(k):
    return (k & ~3) | ((k & 1) << 1) | ((k >> 1) & 1)


def pack_body(
    dest_hbm,
    item_hbm,
    words_hbm,
    rows_hbm,
    cot_hbm,
    pack_ref,
    inc_ref,
    send_ref,
    dest_ref,
    item_ref,
    words_ref,
    rows_ref,
    turned_ref,
    sems,
    *,
    half,
    members,
    groups,
):
    items = rows_ref.shape[0]
    tiles = dest_ref.shape[0]
    core = lax.axis_index("mp")
    place = lax.axis_index("shard") % groups
    start = pl.multiple_of(core * half, half)
    rows = send_ref.shape[0]
    theirs = pl.ds(pl.multiple_of((1 - core) * rows, rows), rows)
    copies = [
        pltpu.make_async_copy(src, dst, sems.at[i])
        for i, (src, dst) in enumerate(
            (
                (words_hbm, words_ref),
                (dest_hbm, dest_ref),
                (item_hbm, item_ref),
                (rows_hbm, rows_ref),
                (cot_hbm.at[theirs, :], send_ref),
            )
        )
    ]
    for copy in copies:
        copy.start()
    copies[0].wait()
    turned_ref[...] = words_ref[...].astype(F32).T
    words = turned_ref[pl.ds(start, half), :].astype(jnp.int32)
    pack_ref[items : items + half, :] = (words & 255).astype(F32).astype(BF16)
    pack_ref[items + half : items + 2 * half, :] = (words >> 8).astype(F32).astype(BF16)
    copies[1].wait()
    copies[2].wait()
    lanes = lax.broadcasted_iota(jnp.int32, (16, pack_ref.shape[1]), 1)
    meta = jnp.zeros_like(lanes)
    for t in range(tiles):
        dest = dest_ref[t]
        hop = (dest % groups) ^ place
        hop = jnp.where(core == 1, crossed(hop), hop)
        slot = hop * members + dest // groups
        meta = jnp.where(lanes == t, slot, meta)
        meta = jnp.where(lanes == tiles + t, item_ref[t], meta)
    pack_ref[items + 2 * half :, :] = meta.astype(F32).astype(BF16)
    inc_ref[...] = pack_ref[items:, :]
    copies[3].wait()
    pack_ref[0:items, :] = rows_ref[...].astype(BF16)
    copies[4].wait()


def spread_body(pack_ref, out_ref):
    source = lax.broadcasted_iota(jnp.int32, (out_ref.shape[0], 2 * BLOCK), 0)
    words = out_ref.shape[0] // 2
    for c in range(0, out_ref.shape[1], 2 * BLOCK):
        target = lax.broadcasted_iota(jnp.int32, (out_ref.shape[0], 2 * BLOCK), 1) + c
        hit = source == (target // 16) + words * ((target // 8) % 2)
        out_ref[:, c : c + 2 * BLOCK] = jnp.where(hit, 1.0, 0.0).astype(BF16)


def join_halves(whole_ref, own_refs, other_ref, items):
    core = lax.axis_index("mp")
    width = other_ref.shape[1]
    rows = items // 2
    mine = pl.ds(pl.multiple_of(core * width, width), width)
    theirs = pl.ds(pl.multiple_of((1 - core) * width, width), width)
    for part, half in ((0, core), (1, 1 - core)):
        at = pl.multiple_of(half * rows, rows)
        for l, own in enumerate(own_refs):
            to = pl.ds((part * len(own_refs) + l) * rows, rows)
            whole_ref[to, mine] = own[pl.ds(at, rows), :]
            whole_ref[to, theirs] = other_ref[pl.ds(l * items + at, rows), :]


def own_first(lane, l, members, rows):
    at = lane - 2 * l * rows
    mine = (at // rows) == lax.axis_index("mp")
    return at % rows + l * rows + jnp.where(mine, 0, members * rows)


def masks_body(idx_ref, *refs, per, half, items, tiles, own):
    incs = refs[:-2]
    spread_ref, mt_ref = refs[-2:]
    first = incs[0].shape[0] - 2 * half - 16
    mt_ref[...] = jnp.zeros_like(mt_ref)
    byte_rows = jnp.concatenate(
        [
            jnp.concatenate(
                [p[first : first + half, :], p[first + half : first + 2 * half, :]], axis=1
            )
            for p in incs
        ],
        axis=0,
    )
    shift = lax.broadcasted_iota(jnp.int32, (len(incs) * half, 2 * BLOCK), 1) % 8
    for q in range(tiles // 2):
        spread = dot(byte_rows, spread_ref[:, q * 2 * BLOCK : (q + 1) * 2 * BLOCK])
        bits = jnp.right_shift(spread.astype(jnp.int32), shift) & 1
        mask = bits.astype(F32).astype(BF16)
        for l in range(len(incs)):
            for b in range(2):
                t = 2 * q + b
                slot = idx_ref[l, t]
                if own:
                    slot = jnp.where(slot // per == l, slot % per, per)
                row = pl.multiple_of(slot * half, half)
                lane = idx_ref[l, tiles + t] * BLOCK + l * items
                if not own:
                    lane = own_first(lane, l, len(incs), items // 2)
                lane = pl.multiple_of(lane, BLOCK)
                where = (pl.ds(row, half), pl.ds(lane, BLOCK))
                mt_ref[where] = (
                    mt_ref[where]
                    + mask[l * half : (l + 1) * half, b * BLOCK : (b + 1) * BLOCK]
                )


def sums_body(mt_ref, *refs, members, items, first):
    rows_ref, out_ref = refs[members + 1 :]
    join_halves(rows_ref, refs[:members], refs[members], items)
    per = out_ref.shape[0]
    total = dot(mt_ref[first * per : (first + 1) * per, :], rows_ref[...])
    out_ref[...] = total.astype(out_ref.dtype)


def sums_rest_body(mt_ref, rows_ref, *out_refs, which):
    per = out_refs[0].shape[0]
    for i, out in zip(which, out_refs):
        total = dot(mt_ref[i * per : (i + 1) * per, :], rows_ref[...])
        out[...] = total.astype(out.dtype)


def grad_own_body(mt_ref, own_ref, out_ref):
    out_ref[...] = dot(mt_ref[:, 0 : own_ref.shape[0]], own_ref[...])


def grad_sums_body(mt_ref, acc_ref, other_ref, *out_refs, which):
    per = out_refs[0].shape[0]
    wide = other_ref.shape[0]
    for i, out in zip(which, out_refs):
        at = slice(i * per, (i + 1) * per)
        total = acc_ref[at, :] + dot(mt_ref[at, wide : 2 * wide], other_ref[...])
        out[...] = total.astype(out.dtype)


def turn_body(mt_ref, out_ref):
    for c in range(0, out_ref.shape[1], BLOCK):
        out_ref[:, c : c + BLOCK] = mt_ref[c : c + BLOCK, :].astype(F32).T.astype(BF16)


def item_hidden_body(mine_ref, other_ref, down_a, down_b, hid_ref, cot_ref):
    core = lax.axis_index("mp")
    width = mine_ref.shape[1]
    rows = other_ref.shape[0]
    cot_ref[:, pl.ds(pl.multiple_of(core * width, width), width)] = mine_ref[
        pl.ds(pl.multiple_of(core * rows, rows), rows), :
    ]
    cot_ref[:, pl.ds(pl.multiple_of((1 - core) * width, width), width)] = other_ref[...]
    cot = cot_ref[...]
    at = 0
    for down in (down_a, down_b):
        for c in range(0, down.shape[0], CHUNK):
            hid_ref[:, at : at + CHUNK] = dot_nt(cot, down[c : c + CHUNK, :])
            at += CHUNK


def add_all(refs):
    total = refs[0][...].astype(F32)
    for r in refs[1:]:
        total = total + r[...].astype(F32)
    return total


def rms(values):
    return lax.rsqrt(jnp.mean(values * values, axis=-1, keepdims=True) + NORM_EPSILON)


def basket_body(*refs, groups):
    parts = refs[:groups]
    gain_ref, gate_a, gate_b, up_a, up_b, down_a, down_b = refs[groups : groups + 7]
    out_ref, sum_ref, value_ref, slope_ref = refs[groups + 7 :]
    total = add_all(parts)
    sum_ref[...] = total
    normed = total * rms(total) * gain_ref[...]
    normed_bf = normed.astype(BF16)
    acc = normed
    at = 0
    for gate, up, down in ((gate_a, up_a, down_a), (gate_b, up_b, down_b)):
        for c in range(0, gate.shape[1], CHUNK):
            gate_pre = dot(normed_bf, gate[:, c : c + CHUNK])
            up_pre = dot(normed_bf, up[:, c : c + CHUNK])
            sig = sigmoid(gate_pre)
            value = gate_pre * sig
            acc = acc + dot((value * up_pre).astype(BF16), down[c : c + CHUNK, :])
            value_ref[:, at : at + CHUNK] = value.astype(BF16)
            slope_ref[:, at : at + CHUNK] = (up_pre * (sig + value * (1.0 - sig))).astype(BF16)
            at += CHUNK
    out_ref[...] = acc.astype(BF16)


def message_body(mo_ref, out_ref, mine_ref, theirs_ref, all_ref, *, peers):
    all_ref[...] = dot(mo_ref[...], out_ref[...])
    rows = mine_ref.shape[0] // peers
    core = lax.axis_index("mp")
    for l in range(peers):
        mine = pl.multiple_of((2 * l + core) * rows, rows)
        theirs = pl.multiple_of((2 * l + 1 - core) * rows, rows)
        mine_ref[l * rows : (l + 1) * rows, :] = all_ref[pl.ds(mine, rows), :]
        to = slice(crossed(l) * rows, (crossed(l) + 1) * rows)
        theirs_ref[to, :] = all_ref[pl.ds(theirs, rows), :].astype(BF16)


def join_body(mine_ref, other_ref, *out_refs):
    rows = out_refs[0].shape[0]
    for l, out in enumerate(out_refs):
        at = slice(l * rows, (l + 1) * rows)
        out[...] = (mine_ref[at, :] + other_ref[at, :].astype(F32)).astype(out.dtype)


def item_body(*refs, peers):
    hidden_ref, gain_ref, gate_a, gate_b, up_a, up_b, out_ref = refs[peers:]
    message = add_all(refs[:peers])
    scale = rms(message)
    gain = gain_ref[...]
    query = (message * scale * gain).astype(BF16)
    acc = jnp.zeros_like(message)
    at = 0
    for gate, up in ((gate_a, up_a), (gate_b, up_b)):
        for c in range(0, gate.shape[1], CHUNK):
            gate_w = gate[:, c : c + CHUNK]
            up_w = up[:, c : c + CHUNK]
            gate_pre = dot(query, gate_w)
            up_pre = dot(query, up_w)
            sig = sigmoid(gate_pre)
            value = gate_pre * sig
            hidden = hidden_ref[:, at : at + CHUNK]
            grad_up = (hidden * value).astype(BF16)
            grad_gate = (hidden * up_pre * (sig + value * (1.0 - sig))).astype(BF16)
            acc = acc + dot_nt(grad_gate, gate_w) + dot_nt(grad_up, up_w)
            at += CHUNK
    weighted = gain * acc
    inner = jnp.mean(weighted * message, axis=1, keepdims=True)
    cubed = scale * scale * scale
    out_ref[...] = (scale * weighted - message * (cubed * inner)).astype(BF16)


def basket_back_body(*refs, groups):
    parts = refs[:groups]
    sum_ref, value_ref, slope_ref, gain_ref = refs[groups : groups + 4]
    gate_a, gate_b, up_a, up_b, down_a, down_b, out_ref = refs[groups + 4 :]
    grad_out = add_all(parts)
    grad_bf = grad_out.astype(BF16)
    acc = grad_out
    at = 0
    for gate, up, down in ((gate_a, up_a, down_a), (gate_b, up_b, down_b)):
        for c in range(0, gate.shape[1], CHUNK):
            hidden = dot_nt(grad_bf, down[c : c + CHUNK, :])
            grad_up = (hidden * value_ref[:, at : at + CHUNK].astype(F32)).astype(BF16)
            grad_gate = (hidden * slope_ref[:, at : at + CHUNK].astype(F32)).astype(BF16)
            acc = acc + dot_nt(grad_gate, gate[:, c : c + CHUNK])
            acc = acc + dot_nt(grad_up, up[:, c : c + CHUNK])
            at += CHUNK
    total = sum_ref[...]
    scale = rms(total)
    weighted = gain_ref[...] * acc
    inner = jnp.mean(weighted * total, axis=1, keepdims=True)
    cubed = scale * scale * scale
    out_ref[...] = (scale * weighted - total * (cubed * inner)).astype(BF16)


def back_body(mo_ref, sum_ref, mine_ref, theirs_ref, all_ref, *, peers):
    all_ref[...] = dot(mo_ref[...], sum_ref[...])
    width = mine_ref.shape[1]
    core = lax.axis_index("mp")
    mine_ref[...] = all_ref[:, pl.ds(pl.multiple_of(core * width, width), width)]
    rows = mine_ref.shape[0] // peers
    theirs = pl.ds(pl.multiple_of((1 - core) * width, width), width)
    for l in range(peers):
        to = slice(crossed(l) * rows, (crossed(l) + 1) * rows)
        theirs_ref[to, :] = all_ref[l * rows : (l + 1) * rows, theirs].astype(BF16)


def adam_body(*refs, peers):
    cot_ref, rows_ref, first_ref, second_ref, r_ref, f_ref, s_ref = refs[peers:]
    gradient = cot_ref[...].astype(F32) + add_all(refs[:peers])
    first = BETA_FIRST * first_ref[...] + (1.0 - BETA_FIRST) * gradient
    second = BETA_SECOND * second_ref[...] + (1.0 - BETA_SECOND) * gradient * gradient
    f_ref[...] = first
    s_ref[...] = second
    r_ref[...] = rows_ref[...] - LEARNING_RATE * first / (jnp.sqrt(second) + ADAM_EPSILON)


def local(
    item_rows,
    first_moment,
    second_moment,
    item_cot,
    tile_bits,
    tile_item,
    tile_dest,
    basket_gain,
    item_gain,
    gate_basket,
    up_basket,
    down_basket,
    gate_item,
    up_item,
    down_item,
):
    shards = lax.axis_size("shard")
    members = GATHER if shards % GATHER == 0 else 1
    groups = shards // members
    items, width = item_rows.shape
    features = basket_gain.shape[0]
    tiles, words, _ = tile_bits.shape
    half = BLOCK // 2
    item_half = items // 2
    hidden = 2 * gate_basket.shape[1]
    per = members * half

    def swap(x):
        return lax.ppermute(x, "mp", [(0, 1), (1, 0)])

    def gather(x):
        got = []
        for k in range(1, members):
            pairs = [(s, ((s // groups) ^ k) * groups + s % groups) for s in range(shards)]
            got.append(lax.ppermute(x, "shard", pairs))
        return got

    def exchange(xs):
        got = [xs[0]]
        for k in range(1, groups):
            pairs = [
                (2 * s + c, 2 * ((s // groups) * groups + ((s % groups) ^ hop)) + c)
                for s in range(shards)
                for c, hop in ((0, k), (1, crossed(k)))
            ]
            got.append(lax.ppermute(xs[k], ("shard", "mp"), pairs))
        return got

    pack, inc, cot_send = run(
        functools.partial(pack_body, half=half, members=members, groups=groups),
        [
            sds((items + 2 * half + 16, width), BF16),
            sds((2 * half + 16, width), BF16),
            sds((item_half, width), BF16),
        ],
        (),
        (),
        far=(tile_dest, tile_item, tile_bits.reshape(tiles * words, BLOCK), item_rows, item_cot),
        scratch=[
            pltpu.SMEM((tiles,), jnp.int32),
            pltpu.SMEM((tiles,), jnp.int32),
            pltpu.VMEM((tiles * words, BLOCK), jnp.int32),
            pltpu.VMEM((items, width), F32),
            pltpu.VMEM((BLOCK, tiles * words), F32),
            pltpu.SemaphoreType.DMA((5,)),
        ],
    )
    packs = [pack] + gather(pack)
    spread = run(
        spread_body, sds((2 * tiles * words, tiles * BLOCK), BF16), (), (pack,), flops=1 << 29
    )
    cot_other = swap(cot_send)
    gate_b, up_b, down_b = gate_basket, up_basket, down_basket
    gate_bo, up_bo, down_bo = swap(gate_basket), swap(up_basket), swap(down_basket)
    rows_other = swap(jnp.concatenate([q[:items] for q in packs], axis=0))
    incs = exchange([inc] * groups)
    metas = [q[items + 2 * half : items + 2 * half + 1] for q in packs]
    idx = jnp.concatenate(metas, axis=0).astype(jnp.int32)
    metas = [q[2 * half : 2 * half + 1] for q in incs]
    idx_plane = jnp.concatenate(metas, axis=0).astype(jnp.int32)

    lead = min(2, groups - 1)
    rest = [i for i in range(groups) if i != lead]
    rest_shapes = [sds((per, features), F32 if i == 0 else BF16) for i in rest]
    mt = run(
        functools.partial(
            masks_body, per=members, half=half, items=items, tiles=tiles, own=False
        ),
        sds((shards * half, members * items), BF16),
        (idx,),
        (*packs, spread),
        flops=1 << 29,
    )
    whole_rows, lead_part = run(
        functools.partial(sums_body, members=members, items=items, first=lead),
        [sds((members * items, features), BF16), sds((per, features), BF16)],
        (),
        (mt, *packs, rows_other),
        flops=1 << 27,
    )
    rest_parts = run(
        functools.partial(sums_rest_body, which=rest),
        rest_shapes,
        (),
        (mt, whole_rows),
        flops=1 << 28,
    )
    parts = dict(zip(rest, rest_parts)) | {lead: lead_part}
    received = exchange(parts)
    mt_plane = run(
        functools.partial(
            masks_body, per=members, half=half, items=items, tiles=tiles, own=True
        ),
        sds(((members + 1) * half, groups * items), BF16),
        (idx_plane,),
        (*incs, spread),
        flops=1 << 29,
    )
    mo = run(turn_body, sds((groups * items, per), BF16), (), (mt_plane,), flops=1 << 28)
    gate_io, up_io, down_io = swap(gate_item), swap(up_item), swap(down_item)
    basket_out, basket_sum, value, slope = run(
        functools.partial(basket_body, groups=groups),
        [
            sds((per, features), BF16),
            sds((per, features), F32),
            sds((per, hidden), BF16),
            sds((per, hidden), BF16),
        ],
        (),
        (
            *received,
            basket_gain.reshape(1, features),
            gate_b,
            gate_bo,
            up_b,
            up_bo,
            down_b,
            down_bo,
        ),
        flops=1 << 30,
    )
    message_mine, message_theirs = run(
        functools.partial(message_body, peers=groups),
        [sds((groups * item_half, features), F32), sds((groups * item_half, features), BF16)],
        (),
        (mo, basket_out),
        scratch=[pltpu.VMEM((groups * items, features), F32)],
        flops=1 << 28,
    )
    message_other = swap(message_theirs)
    item_hidden = run(
        item_hidden_body,
        sds((item_half, hidden), F32),
        (),
        (item_cot, cot_other, down_item, down_io),
        scratch=[pltpu.VMEM((item_half, features), BF16)],
        flops=1 << 29,
    )
    messages = run(
        join_body,
        [sds((item_half, features), F32)] + [sds((item_half, features), BF16)] * (groups - 1),
        (),
        (message_mine, message_other),
    )
    grad_message = run(
        functools.partial(item_body, peers=groups),
        sds((item_half, features), BF16),
        (),
        (
            *exchange(messages),
            item_hidden,
            item_gain.reshape(1, features),
            gate_item,
            gate_io,
            up_item,
            up_io,
        ),
        flops=1 << 30,
    )
    grads = [grad_message] + gather(grad_message)
    grads = jnp.concatenate(grads, axis=0)
    grads_other = swap(grads)
    grad_acc = run(
        grad_own_body, sds((shards * half, features), F32), (), (mt, grads), flops=1 << 28
    )
    (lead_part,) = run(
        functools.partial(grad_sums_body, which=[lead]),
        [sds((per, features), BF16)],
        (),
        (mt, grad_acc, grads_other),
        flops=1 << 27,
    )
    rest_parts = run(
        functools.partial(grad_sums_body, which=rest),
        rest_shapes,
        (),
        (mt, grad_acc, grads_other),
        flops=1 << 28,
    )
    grad_parts = dict(zip(rest, rest_parts)) | {lead: lead_part}
    grad_received = exchange(grad_parts)
    grad_sum = run(
        functools.partial(basket_back_body, groups=groups),
        sds((per, features), BF16),
        (),
        (
            *grad_received,
            basket_sum,
            value,
            slope,
            basket_gain.reshape(1, features),
            gate_b,
            gate_bo,
            up_b,
            up_bo,
            down_b,
            down_bo,
        ),
        flops=1 << 30,
    )
    back_mine, back_theirs = run(
        functools.partial(back_body, peers=groups),
        [sds((groups * items, width), F32), sds((groups * items, width), BF16)],
        (),
        (mo, grad_sum),
        scratch=[pltpu.VMEM((groups * items, features), F32)],
        flops=1 << 28,
    )
    back_other = swap(back_theirs)
    backs = run(
        join_body,
        [sds((items, width), F32)] + [sds((items, width), BF16)] * (groups - 1),
        (),
        (back_mine, back_other),
    )
    new_rows, new_first, new_second = run(
        functools.partial(adam_body, peers=groups),
        [sds((items, width), F32)] * 3,
        (),
        (*exchange(backs), item_cot, item_rows, first_moment, second_moment),
    )
    return (new_rows, new_first, new_second)


def solution(mesh):
    return jax.shard_map(
        local,
        mesh=mesh,
        in_specs=(
            P("shard", "mp"),
            P("shard", "mp"),
            P("shard", "mp"),
            P("shard", "mp"),
            P("shard", None, None),
            P("shard"),
            P("shard"),
            P(),
            P(),
            P(None, "mp"),
            P(None, "mp"),
            P("mp", None),
            P(None, "mp"),
            P(None, "mp"),
            P("mp", None),
        ),
        out_specs=(P("shard", "mp"), P("shard", "mp"), P("shard", "mp")),
        check_vma=False,
    )
```

```python
import functools

import jax
import jax.numpy as jnp
import numpy as np
from jax import lax
from jax.experimental import pallas as pl
from jax.experimental.pallas import tpu as pltpu
from jax.sharding import PartitionSpec as P


BLOCK = 128
GATHER = 4
CHUNK = 1024

NORM_EPSILON = 1e-05
LEARNING_RATE = 0.01
BETA_FIRST = 0.9
BETA_SECOND = 0.99
ADAM_EPSILON = 1e-08


F32 = jnp.float32
BF16 = jnp.bfloat16


def sds(shape, dtype):
    return jax.ShapeDtypeStruct(shape, dtype)


def nbytes(x):
    return int(np.prod(x.shape)) * jnp.dtype(x.dtype).itemsize


def run(body, outs, smem, args, scratch=(), flops=1 << 20, far=(), limit=0):
    held = [x for x in scratch if isinstance(x.dtype, np.dtype) or x.dtype in (F32, BF16)]
    limit = limit or sum(nbytes(x) for x in (*args, *jax.tree.leaves(outs), *held)) + (4 << 20)
    specs = [pl.BlockSpec(memory_space=pltpu.HBM)] * len(far)
    specs += [pl.BlockSpec(memory_space=pltpu.SMEM)] * len(smem)
    specs += [pl.BlockSpec(memory_space=pltpu.VMEM)] * len(args)
    call = pl.pallas_call(
        body,
        out_shape=outs,
        in_specs=specs,
        out_specs=jax.tree.map(lambda _: pl.BlockSpec(memory_space=pltpu.VMEM), outs),
        scratch_shapes=list(scratch),
        cost_estimate=pl.CostEstimate(flops=flops, bytes_accessed=1 << 20, transcendentals=0),
        compiler_params=pltpu.CompilerParams(vmem_limit_bytes=min(limit, 60 * 1024 * 1024)),
    )
    far = [pltpu.with_memory_space_constraint(x, pltpu.HBM) for x in far]
    return call(*far, *smem, *args)


def dot(a, b):
    return jnp.dot(a, b, preferred_element_type=F32)


def dot_nt(a, b):
    return lax.dot_general(a, b, (((1,), (1,)), ((), ())), preferred_element_type=F32)


def sigmoid(v):
    return 0.5 * jnp.tanh(0.5 * v) + 0.5


def crossed(k):
    return (k & ~3) | ((k & 1) << 1) | ((k >> 1) & 1)


def pack_body(
    dest_hbm,
    item_hbm,
    words_hbm,
    rows_hbm,
    cot_hbm,
    pack_ref,
    inc_ref,
    send_ref,
    dest_ref,
    item_ref,
    words_ref,
    rows_ref,
    turned_ref,
    sems,
    *,
    half,
    members,
    groups,
):
    items = rows_ref.shape[0]
    tiles = dest_ref.shape[0]
    core = lax.axis_index("mp")
    place = lax.axis_index("shard") % groups
    start = pl.multiple_of(core * half, half)
    rows = send_ref.shape[0]
    theirs = pl.ds(pl.multiple_of((1 - core) * rows, rows), rows)
    copies = [
        pltpu.make_async_copy(src, dst, sems.at[i])
        for i, (src, dst) in enumerate(
            (
                (words_hbm, words_ref),
                (dest_hbm, dest_ref),
                (item_hbm, item_ref),
                (rows_hbm, rows_ref),
                (cot_hbm.at[theirs, :], send_ref),
            )
        )
    ]
    for copy in copies:
        copy.start()
    copies[0].wait()
    turned_ref[...] = words_ref[...].astype(F32).T
    words = turned_ref[pl.ds(start, half), :].astype(jnp.int32)
    pack_ref[items : items + half, :] = (words & 255).astype(F32).astype(BF16)
    pack_ref[items + half : items + 2 * half, :] = (words >> 8).astype(F32).astype(BF16)
    copies[1].wait()
    copies[2].wait()
    lanes = lax.broadcasted_iota(jnp.int32, (16, pack_ref.shape[1]), 1)
    meta = jnp.zeros_like(lanes)
    for t in range(tiles):
        dest = dest_ref[t]
        hop = (dest % groups) ^ place
        hop = jnp.where(core == 1, crossed(hop), hop)
        slot = hop * members + dest // groups
        meta = jnp.where(lanes == t, slot, meta)
        meta = jnp.where(lanes == tiles + t, item_ref[t], meta)
    pack_ref[items + 2 * half :, :] = meta.astype(F32).astype(BF16)
    inc_ref[...] = pack_ref[items:, :]
    copies[3].wait()
    pack_ref[0:items, :] = rows_ref[...].astype(BF16)
    copies[4].wait()


def spread_body(pack_ref, out_ref):
    source = lax.broadcasted_iota(jnp.int32, (out_ref.shape[0], 2 * BLOCK), 0)
    words = out_ref.shape[0] // 2
    for c in range(0, out_ref.shape[1], 2 * BLOCK):
        target = lax.broadcasted_iota(jnp.int32, (out_ref.shape[0], 2 * BLOCK), 1) + c
        hit = source == (target // 16) + words * ((target // 8) % 2)
        out_ref[:, c : c + 2 * BLOCK] = jnp.where(hit, 1.0, 0.0).astype(BF16)


def join_halves(whole_ref, own_refs, other_ref, items):
    core = lax.axis_index("mp")
    width = other_ref.shape[1]
    rows = items // 2
    mine = pl.ds(pl.multiple_of(core * width, width), width)
    theirs = pl.ds(pl.multiple_of((1 - core) * width, width), width)
    for part, half in ((0, core), (1, 1 - core)):
        at = pl.multiple_of(half * rows, rows)
        for l, own in enumerate(own_refs):
            to = pl.ds((part * len(own_refs) + l) * rows, rows)
            whole_ref[to, mine] = own[pl.ds(at, rows), :]
            whole_ref[to, theirs] = other_ref[pl.ds(l * items + at, rows), :]


def own_first(lane, l, members, rows):
    at = lane - 2 * l * rows
    mine = (at // rows) == lax.axis_index("mp")
    return at % rows + l * rows + jnp.where(mine, 0, members * rows)


def masks_body(idx_ref, *refs, per, half, items, tiles, own):
    incs = refs[:-2]
    spread_ref, mt_ref = refs[-2:]
    first = incs[0].shape[0] - 2 * half - 16
    mt_ref[...] = jnp.zeros_like(mt_ref)
    byte_rows = jnp.concatenate(
        [
            jnp.concatenate(
                [p[first : first + half, :], p[first + half : first + 2 * half, :]], axis=1
            )
            for p in incs
        ],
        axis=0,
    )
    shift = lax.broadcasted_iota(jnp.int32, (len(incs) * half, 2 * BLOCK), 1) % 8
    for q in range(tiles // 2):
        spread = dot(byte_rows, spread_ref[:, q * 2 * BLOCK : (q + 1) * 2 * BLOCK])
        bits = jnp.right_shift(spread.astype(jnp.int32), shift) & 1
        mask = bits.astype(F32).astype(BF16)
        for l in range(len(incs)):
            for b in range(2):
                t = 2 * q + b
                slot = idx_ref[l, t]
                if own:
                    slot = jnp.where(slot // per == l, slot % per, per)
                row = pl.multiple_of(slot * half, half)
                lane = idx_ref[l, tiles + t] * BLOCK + l * items
                if not own:
                    lane = own_first(lane, l, len(incs), items // 2)
                lane = pl.multiple_of(lane, BLOCK)
                where = (pl.ds(row, half), pl.ds(lane, BLOCK))
                mt_ref[where] = (
                    mt_ref[where]
                    + mask[l * half : (l + 1) * half, b * BLOCK : (b + 1) * BLOCK]
                )


def sums_body(mt_ref, *refs, members, items, first):
    rows_ref, out_ref = refs[members + 1 :]
    join_halves(rows_ref, refs[:members], refs[members], items)
    per = out_ref.shape[0]
    total = dot(mt_ref[first * per : (first + 1) * per, :], rows_ref[...])
    out_ref[...] = total.astype(out_ref.dtype)


def sums_rest_body(mt_ref, rows_ref, *out_refs, which):
    per = out_refs[0].shape[0]
    for i, out in zip(which, out_refs):
        total = dot(mt_ref[i * per : (i + 1) * per, :], rows_ref[...])
        out[...] = total.astype(out.dtype)


def grad_own_body(mt_ref, own_ref, out_ref):
    out_ref[...] = dot(mt_ref[:, 0 : own_ref.shape[0]], own_ref[...])


def grad_sums_body(mt_ref, acc_ref, other_ref, *out_refs, which):
    per = out_refs[0].shape[0]
    wide = other_ref.shape[0]
    for i, out in zip(which, out_refs):
        at = slice(i * per, (i + 1) * per)
        total = acc_ref[at, :] + dot(mt_ref[at, wide : 2 * wide], other_ref[...])
        out[...] = total.astype(out.dtype)


def turn_body(mt_ref, out_ref):
    for c in range(0, out_ref.shape[1], BLOCK):
        out_ref[:, c : c + BLOCK] = mt_ref[c : c + BLOCK, :].astype(F32).T.astype(BF16)


def item_hidden_body(mine_ref, other_ref, down_a, down_b, hid_ref, cot_ref):
    core = lax.axis_index("mp")
    width = mine_ref.shape[1]
    rows = other_ref.shape[0]
    cot_ref[:, pl.ds(pl.multiple_of(core * width, width), width)] = mine_ref[
        pl.ds(pl.multiple_of(core * rows, rows), rows), :
    ]
    cot_ref[:, pl.ds(pl.multiple_of((1 - core) * width, width), width)] = other_ref[...]
    cot = cot_ref[...]
    at = 0
    for down in (down_a, down_b):
        for c in range(0, down.shape[0], CHUNK):
            hid_ref[:, at : at + CHUNK] = dot_nt(cot, down[c : c + CHUNK, :])
            at += CHUNK


def add_all(refs):
    total = refs[0][...].astype(F32)
    for r in refs[1:]:
        total = total + r[...].astype(F32)
    return total


def rms(values):
    return lax.rsqrt(jnp.mean(values * values, axis=-1, keepdims=True) + NORM_EPSILON)


def basket_body(*refs, groups):
    parts = refs[:groups]
    gain_ref, gate_a, gate_b, up_a, up_b, down_a, down_b = refs[groups : groups + 7]
    out_ref, sum_ref, gate_ref, up_ref = refs[groups + 7 :]
    total = add_all(parts)
    sum_ref[...] = total
    normed = total * rms(total) * gain_ref[...]
    normed_bf = normed.astype(BF16)
    acc = normed
    at = 0
    for gate, up, down in ((gate_a, up_a, down_a), (gate_b, up_b, down_b)):
        for c in range(0, gate.shape[1], CHUNK):
            gate_pre = dot(normed_bf, gate[:, c : c + CHUNK])
            up_pre = dot(normed_bf, up[:, c : c + CHUNK])
            sig = sigmoid(gate_pre)
            value = gate_pre * sig
            acc = acc + dot((value * up_pre).astype(BF16), down[c : c + CHUNK, :])
            gate_ref[:, at : at + CHUNK] = gate_pre
            up_ref[:, at : at + CHUNK] = up_pre
            at += CHUNK
    out_ref[...] = acc.astype(BF16)


def slopes_body(gate_ref, up_ref, value_ref, slope_ref):
    for c in range(0, gate_ref.shape[1], 256):
        gate_pre = gate_ref[:, c : c + 256]
        sig = sigmoid(gate_pre)
        value = gate_pre * sig
        value_ref[:, c : c + 256] = value.astype(BF16)
        slope = up_ref[:, c : c + 256] * (sig + value * (1.0 - sig))
        slope_ref[:, c : c + 256] = slope.astype(BF16)


def message_theirs_body(mo_ref, out_ref, theirs_ref, *, peers):
    rows = theirs_ref.shape[0] // peers
    core = lax.axis_index("mp")
    for l in range(peers):
        at = pl.ds(pl.multiple_of((2 * l + 1 - core) * rows, rows), rows)
        to = slice(crossed(l) * rows, (crossed(l) + 1) * rows)
        theirs_ref[to, :] = dot(mo_ref[at, :], out_ref[...]).astype(BF16)


def message_mine_body(mo_ref, out_ref, mine_ref, *, peers):
    rows = mine_ref.shape[0] // peers
    core = lax.axis_index("mp")
    for l in range(peers):
        at = pl.ds(pl.multiple_of((2 * l + core) * rows, rows), rows)
        mine_ref[l * rows : (l + 1) * rows, :] = dot(mo_ref[at, :], out_ref[...])


def join_body(mine_ref, other_ref, *out_refs):
    rows = out_refs[0].shape[0]
    for l, out in enumerate(out_refs):
        at = slice(l * rows, (l + 1) * rows)
        out[...] = (mine_ref[at, :] + other_ref[at, :].astype(F32)).astype(out.dtype)


def item_body(*refs, peers):
    hidden_ref, gain_ref, gate_a, gate_b, up_a, up_b, out_ref = refs[peers:]
    message = add_all(refs[:peers])
    scale = rms(message)
    gain = gain_ref[...]
    query = (message * scale * gain).astype(BF16)
    acc = jnp.zeros_like(message)
    at = 0
    for gate, up in ((gate_a, up_a), (gate_b, up_b)):
        for c in range(0, gate.shape[1], CHUNK):
            gate_w = gate[:, c : c + CHUNK]
            up_w = up[:, c : c + CHUNK]
            gate_pre = dot(query, gate_w)
            up_pre = dot(query, up_w)
            sig = sigmoid(gate_pre)
            value = gate_pre * sig
            hidden = hidden_ref[:, at : at + CHUNK]
            grad_up = (hidden * value).astype(BF16)
            grad_gate = (hidden * up_pre * (sig + value * (1.0 - sig))).astype(BF16)
            acc = acc + dot_nt(grad_gate, gate_w) + dot_nt(grad_up, up_w)
            at += CHUNK
    weighted = gain * acc
    inner = jnp.mean(weighted * message, axis=1, keepdims=True)
    cubed = scale * scale * scale
    out_ref[...] = (scale * weighted - message * (cubed * inner)).astype(BF16)


def basket_back_body(*refs, groups):
    parts = refs[:groups]
    sum_ref, value_ref, slope_ref, gain_ref = refs[groups : groups + 4]
    gate_a, gate_b, up_a, up_b, down_a, down_b, out_ref = refs[groups + 4 :]
    grad_out = add_all(parts)
    grad_bf = grad_out.astype(BF16)
    acc = grad_out
    at = 0
    for gate, up, down in ((gate_a, up_a, down_a), (gate_b, up_b, down_b)):
        for c in range(0, gate.shape[1], CHUNK):
            hidden = dot_nt(grad_bf, down[c : c + CHUNK, :])
            grad_up = (hidden * value_ref[:, at : at + CHUNK].astype(F32)).astype(BF16)
            grad_gate = (hidden * slope_ref[:, at : at + CHUNK].astype(F32)).astype(BF16)
            acc = acc + dot_nt(grad_gate, gate[:, c : c + CHUNK])
            acc = acc + dot_nt(grad_up, up[:, c : c + CHUNK])
            at += CHUNK
    total = sum_ref[...]
    scale = rms(total)
    weighted = gain_ref[...] * acc
    inner = jnp.mean(weighted * total, axis=1, keepdims=True)
    cubed = scale * scale * scale
    out_ref[...] = (scale * weighted - total * (cubed * inner)).astype(BF16)


def back_theirs_body(mo_ref, sum_ref, theirs_ref, *, peers):
    width = theirs_ref.shape[1]
    core = lax.axis_index("mp")
    rows = theirs_ref.shape[0] // peers
    wanted = sum_ref[:, pl.ds(pl.multiple_of((1 - core) * width, width), width)]
    for l in range(peers):
        to = slice(crossed(l) * rows, (crossed(l) + 1) * rows)
        theirs_ref[to, :] = dot(mo_ref[l * rows : (l + 1) * rows, :], wanted).astype(BF16)


def back_mine_body(mo_ref, sum_ref, mine_ref):
    width = mine_ref.shape[1]
    core = lax.axis_index("mp")
    wanted = sum_ref[:, pl.ds(pl.multiple_of(core * width, width), width)]
    mine_ref[...] = dot(mo_ref[...], wanted)


def adam_body(*refs, peers):
    cot_ref, rows_ref, first_ref, second_ref, r_ref, f_ref, s_ref = refs[peers:]
    gradient = cot_ref[...].astype(F32) + add_all(refs[:peers])
    first = BETA_FIRST * first_ref[...] + (1.0 - BETA_FIRST) * gradient
    second = BETA_SECOND * second_ref[...] + (1.0 - BETA_SECOND) * gradient * gradient
    f_ref[...] = first
    s_ref[...] = second
    r_ref[...] = rows_ref[...] - LEARNING_RATE * first / (jnp.sqrt(second) + ADAM_EPSILON)


def local(
    item_rows,
    first_moment,
    second_moment,
    item_cot,
    tile_bits,
    tile_item,
    tile_dest,
    basket_gain,
    item_gain,
    gate_basket,
    up_basket,
    down_basket,
    gate_item,
    up_item,
    down_item,
):
    shards = lax.axis_size("shard")
    members = GATHER if shards % GATHER == 0 else 1
    groups = shards // members
    items, width = item_rows.shape
    features = basket_gain.shape[0]
    tiles, words, _ = tile_bits.shape
    half = BLOCK // 2
    item_half = items // 2
    hidden = 2 * gate_basket.shape[1]
    per = members * half

    def swap(x):
        return lax.ppermute(x, "mp", [(0, 1), (1, 0)])

    def gather(x):
        got = []
        for k in range(1, members):
            pairs = [(s, ((s // groups) ^ k) * groups + s % groups) for s in range(shards)]
            got.append(lax.ppermute(x, "shard", pairs))
        return got

    def exchange(xs):
        got = [xs[0]]
        for k in range(1, groups):
            pairs = [
                (2 * s + c, 2 * ((s // groups) * groups + ((s % groups) ^ hop)) + c)
                for s in range(shards)
                for c, hop in ((0, k), (1, crossed(k)))
            ]
            got.append(lax.ppermute(xs[k], ("shard", "mp"), pairs))
        return got

    pack, inc, cot_send = run(
        functools.partial(pack_body, half=half, members=members, groups=groups),
        [
            sds((items + 2 * half + 16, width), BF16),
            sds((2 * half + 16, width), BF16),
            sds((item_half, width), BF16),
        ],
        (),
        (),
        far=(tile_dest, tile_item, tile_bits.reshape(tiles * words, BLOCK), item_rows, item_cot),
        scratch=[
            pltpu.SMEM((tiles,), jnp.int32),
            pltpu.SMEM((tiles,), jnp.int32),
            pltpu.VMEM((tiles * words, BLOCK), jnp.int32),
            pltpu.VMEM((items, width), F32),
            pltpu.VMEM((BLOCK, tiles * words), F32),
            pltpu.SemaphoreType.DMA((5,)),
        ],
    )
    packs = [pack] + gather(pack)
    spread = run(
        spread_body,
        sds((2 * tiles * words, tiles * BLOCK), BF16),
        (),
        (pack,),
        flops=1 << 29,
    )
    cot_other = swap(cot_send)
    gate_b, up_b, down_b = gate_basket, up_basket, down_basket
    gate_bo, up_bo, down_bo = swap(gate_basket), swap(up_basket), swap(down_basket)
    rows_other = swap(jnp.concatenate([q[:items] for q in packs], axis=0))
    incs = exchange([inc] * groups)
    metas = [q[items + 2 * half : items + 2 * half + 1] for q in packs]
    idx = jnp.concatenate(metas, axis=0).astype(jnp.int32)
    metas = [q[2 * half : 2 * half + 1] for q in incs]
    idx_plane = jnp.concatenate(metas, axis=0).astype(jnp.int32)

    lead = min(2, groups - 1)
    rest = [i for i in range(groups) if i != lead]
    rest_shapes = [sds((per, features), F32 if i == 0 else BF16) for i in rest]
    mt = run(
        functools.partial(
            masks_body, per=members, half=half, items=items, tiles=tiles, own=False
        ),
        sds((shards * half, members * items), BF16),
        (idx,),
        (*packs, spread),
        flops=1 << 29,
    )
    whole_rows, lead_part = run(
        functools.partial(sums_body, members=members, items=items, first=lead),
        [sds((members * items, features), BF16), sds((per, features), BF16)],
        (),
        (mt, *packs, rows_other),
        flops=1 << 27,
    )
    rest_parts = run(
        functools.partial(sums_rest_body, which=rest),
        rest_shapes,
        (),
        (mt, whole_rows),
        flops=1 << 28,
    )
    parts = dict(zip(rest, rest_parts)) | {lead: lead_part}
    received = exchange(parts)
    mt_plane = run(
        functools.partial(
            masks_body, per=members, half=half, items=items, tiles=tiles, own=True
        ),
        sds(((members + 1) * half, groups * items), BF16),
        (idx_plane,),
        (*incs, spread),
        flops=1 << 29,
    )
    mo = run(
        turn_body, sds((groups * items, per), BF16), (), (mt_plane,), flops=1 << 28
    )
    gate_io, up_io, down_io = swap(gate_item), swap(up_item), swap(down_item)
    basket_out, basket_sum, gate_pre, up_pre = run(
        functools.partial(basket_body, groups=groups),
        [
            sds((per, features), BF16),
            sds((per, features), F32),
            sds((per, hidden), F32),
            sds((per, hidden), F32),
        ],
        (),
        (
            *received,
            basket_gain.reshape(1, features),
            gate_b,
            gate_bo,
            up_b,
            up_bo,
            down_b,
            down_bo,
        ),
        flops=1 << 30,
    )
    value, slope = run(
        slopes_body,
        [sds((per, hidden), BF16)] * 2,
        (),
        (gate_pre, up_pre),
        flops=1 << 29,
    )
    message_theirs = run(
        functools.partial(message_theirs_body, peers=groups),
        sds((groups * item_half, features), BF16),
        (),
        (mo, basket_out),
        flops=1 << 27,
    )
    message_mine = run(
        functools.partial(message_mine_body, peers=groups),
        sds((groups * item_half, features), F32),
        (),
        (mo, basket_out),
        flops=1 << 27,
    )
    message_other = swap(message_theirs)
    item_hidden = run(
        item_hidden_body,
        sds((item_half, hidden), F32),
        (),
        (item_cot, cot_other, down_item, down_io),
        scratch=[pltpu.VMEM((item_half, features), BF16)],
        flops=1 << 29,
    )
    messages = run(
        join_body,
        [sds((item_half, features), F32)] + [sds((item_half, features), BF16)] * (groups - 1),
        (),
        (message_mine, message_other),
    )
    grad_message = run(
        functools.partial(item_body, peers=groups),
        sds((item_half, features), BF16),
        (),
        (
            *exchange(messages),
            item_hidden,
            item_gain.reshape(1, features),
            gate_item,
            gate_io,
            up_item,
            up_io,
        ),
        flops=1 << 30,
    )
    grads = [grad_message] + gather(grad_message)
    grads = jnp.concatenate(grads, axis=0)
    grads_other = swap(grads)
    grad_acc = run(
        grad_own_body,
        sds((shards * half, features), F32),
        (),
        (mt, grads),
        flops=1 << 28,
    )
    (lead_part,) = run(
        functools.partial(grad_sums_body, which=[lead]),
        [sds((per, features), BF16)],
        (),
        (mt, grad_acc, grads_other),
        flops=1 << 27,
    )
    rest_parts = run(
        functools.partial(grad_sums_body, which=rest),
        rest_shapes,
        (),
        (mt, grad_acc, grads_other),
        flops=1 << 28,
    )
    grad_parts = dict(zip(rest, rest_parts)) | {lead: lead_part}
    grad_received = exchange(grad_parts)
    grad_sum = run(
        functools.partial(basket_back_body, groups=groups),
        sds((per, features), BF16),
        (),
        (
            *grad_received,
            basket_sum,
            value,
            slope,
            basket_gain.reshape(1, features),
            gate_b,
            gate_bo,
            up_b,
            up_bo,
            down_b,
            down_bo,
        ),
        flops=1 << 30,
    )
    back_theirs = run(
        functools.partial(back_theirs_body, peers=groups),
        sds((groups * items, width), BF16),
        (),
        (mo, grad_sum),
        flops=1 << 27,
    )
    back_mine = run(
        back_mine_body,
        sds((groups * items, width), F32),
        (),
        (mo, grad_sum),
        flops=1 << 27,
    )
    back_other = swap(back_theirs)
    backs = run(
        join_body,
        [sds((items, width), F32)] + [sds((items, width), BF16)] * (groups - 1),
        (),
        (back_mine, back_other),
    )
    new_rows, new_first, new_second = run(
        functools.partial(adam_body, peers=groups),
        [sds((items, width), F32)] * 3,
        (),
        (*exchange(backs), item_cot, item_rows, first_moment, second_moment),
    )
    return (new_rows, new_first, new_second)


def solution(mesh):
    return jax.shard_map(
        local,
        mesh=mesh,
        in_specs=(
            P("shard", "mp"),
            P("shard", "mp"),
            P("shard", "mp"),
            P("shard", "mp"),
            P("shard", None, None),
            P("shard"),
            P("shard"),
            P(),
            P(),
            P(None, "mp"),
            P(None, "mp"),
            P("mp", None),
            P(None, "mp"),
            P(None, "mp"),
            P("mp", None),
        ),
        out_specs=(P("shard", "mp"), P("shard", "mp"), P("shard", "mp")),
        check_vma=False,
    )
```
